32 devices in a mesh: morton: 8 (over z, x), level: 4 (over y, core).
Axes of the slice: x: 2, y: 2, z: 4, core: 2. Of those that a mesh axis runs over, the one named last changes fastest.
Arguments:
- coarse_density: float32 [4096, 128], P('morton'), may hold values from 0.000125 to 0.12
- coarse_emission: float32 [4096, 128], P('morton'), may hold values from 0 to 4
- fine_density: float32 [16384, 128], P(('morton', 'level')), may hold values from 0.000125 to 0.12
- fine_emission: float32 [16384, 128], P(('morton', 'level')), may hold values from 0 to 4
- coarse_brick: int32 [32768], P(('morton', 'level')), may hold values from 0 to 15
- coarse_lane: int32 [32768], P(('morton', 'level')), may hold values from 0 to 1023
- coarse_entry: int32 [32768], P(('morton', 'level')), may hold values from 0 to 31, as said below
- coarse_count: int32 [32768], P(('morton', 'level')), may hold values from 0 to 32, as said below
- fine_owner: int32 [262144, 1], P(('morton', 'level')), may hold values from 0 to 31; in each aligned block of 8192 rows (0 to 8191, 8192 to 16383, ...) at most 512 rows name the same one
- fine_brick: int32 [262144], P(('morton', 'level')), may hold values from 0 to 1
- fine_lane: int32 [262144], P(('morton', 'level')), may hold values from 0 to 1023
- fine_entry: int32 [262144], P(('morton', 'level')), may hold values from 0 to 31, as said below
- fine_count: int32 [262144], P(('morton', 'level')), may hold values from 0 to 32, as said below
Outputs:
- image_color: float32 [8192], P(('morton', 'level'))
- transmittance: float32 [8192], P(('morton', 'level'))
The draws below stay inside these ranges and needn't reach their ends.
Inputs may be any that keep to these rules, and one draw needn't show every extreme that they name: `coarse_entry`: entry plus count is at most 32 for each segment. `coarse_count`: count 0 marks an empty segment. `fine_entry`: entry plus count is at most 32 for each segment. `fine_count`: count 0 marks a padded slot. `fine_owner`: among the fine segments of one device, at most 512 name one owner device, a bound that some block reaches.
All inputs are finite; a program needn't handle non-finite values.
Results may differ from the reference program's by a relative error of at most 0.0003.
Values sent between devices are 32-bit elements; how exact they have to be, the bound alone decides.
A program may use at most 64 MiB of HBM per device.

```python
import math
import jax
import jax.numpy as jnp
import numpy as np
from jax import lax

BRICK = 32
BROWS = 256
FB = 2
CB = 16
GROUP_PIX = 1024
FSEG = 8
RCAP = 512
SLABSEG = 32768
SEGT = 262144
FINE = 64
N_MORTON = 8
N_LEVEL = 4


def entry_and_count(key, salt, total):
    inner = jax.random.fold_in(key, salt)
    first_key, second_key = jax.random.split(inner)
    entry_ids = jax.random.randint(first_key, (total,), 0, BRICK)
    count_ids = jax.random.randint(second_key, (total,), 0, BRICK - entry_ids + 1)
    return (entry_ids.astype(jnp.int32), count_ids.astype(jnp.int32))


def density_field(key, bricks):
    inner = jax.random.fold_in(key, 29)
    scale_key, cell_key = jax.random.split(inner)
    brick_scale = jnp.exp(jax.random.uniform(scale_key, (bricks, 1, 1), jnp.float32, math.log(0.0005), math.log(0.03)))
    cell_factor = jnp.exp(jax.random.uniform(cell_key, (bricks, BROWS, 128), jnp.float32, math.log(0.25), math.log(4.0)))
    return (brick_scale * cell_factor).reshape(bricks * BROWS, 128).astype(jnp.float32)


def draw_coarse_density(key, part):
    return density_field(key, CB)


def draw_fine_density(key, part):
    return density_field(key, FINE)


def draw_coarse_entry(key, part):
    return entry_and_count(key, 13, SLABSEG)[0]


def draw_coarse_count(key, part):
    return entry_and_count(key, 13, SLABSEG)[1]


def draw_fine_entry(key, part):
    return entry_and_count(key, 11, SEGT)[0]


def draw_fine_count(key, part):
    return entry_and_count(key, 11, SEGT)[1]


def touch_ends(drawn, stream_key, smallest, largest):
    place = [jax.random.randint(jax.random.fold_in(stream_key, axis), (), 0, length) for axis, length in enumerate(drawn.shape)]
    longest = drawn.shape.index(max(drawn.shape))
    beside = place[:longest] + [(place[longest] + 1) % drawn.shape[longest]] + place[longest + 1:]
    return drawn.at[tuple(place)].set(smallest).at[tuple(beside)].set(largest)


def steps_of(own_key, dims, shards, least, high):
    def one(axis_at, shards_of):
        heights = jax.random.uniform(jax.random.fold_in(jax.random.fold_in(own_key, 6), axis_at), (shards_of,), jnp.float32, least / len(shards), high / len(shards))
        return jnp.repeat(jnp.exp(heights), dims[axis_at] // shards_of).reshape((-1,) + (1,) * (len(dims) - axis_at - 1))

    factor_of = one(*shards[0])
    for cut in shards[1:]:
        factor_of = factor_of * one(*cut)
    return factor_of


def routed_block(stream_key, own, number, rows, amount, top, reach, lean):
    ranking = jax.random.permutation(stream_key, amount)
    crowded, common = shares(amount, rows * top, reach, lean, True), shares(amount, rows * top, reach, lean, False)
    places = jnp.arange(amount)

    def named(sizes, offset_by):
        used = int((sizes > 0).sum())
        fixed = max(1, used // 4)
        passed = fixed + (places - fixed + offset_by * (used - fixed)) % max(1, amount - fixed)
        return jnp.zeros((amount,), jnp.int32).at[ranking[jnp.where(places < fixed, places, passed)]].set(jnp.asarray(sizes, jnp.int32))

    sizes = jnp.where(number % 4 == 0, named(crowded, number // 4), named(common, number - number // 4 - 1))
    mixed = jax.random.permutation(jax.random.fold_in(own, 3), amount)
    giver, taker = mixed[0:amount // 2 * 2:2], mixed[1:amount // 2 * 2:2]
    slack = jnp.minimum(sizes[giver] - 1, reach - sizes[taker]) // 2
    slack = jnp.where((giver == ranking[0]) | (taker == ranking[0]) | (sizes[taker] == 0), 0, jnp.maximum(slack, 0))
    passed = jax.random.randint(jax.random.fold_in(own, 4), (amount // 2,), 0, 1 << 20) % (slack + 1)
    sizes = sizes.at[giver].add(-passed).at[taker].add(passed)
    items = jnp.searchsorted(jnp.cumsum(sizes), jnp.arange(rows * top), side="right").astype(jnp.int32)
    listing = items.reshape(top, rows).T
    listing = listing[jax.random.permutation(jax.random.fold_in(own, 1), rows)]
    offset_by = jax.random.randint(jax.random.fold_in(own, 2), (rows, 1), 0, top)
    return jnp.take_along_axis(listing, (jnp.arange(top)[None, :] + offset_by) % top, axis=1)


def shares(amount, total, bound, skew, full):
    loads = [(1 << 20) // math.isqrt(standing ** skew) + 1 for standing in range(1, amount + 1)]
    largest = bound if full else min(bound, max(-(-total // amount), total * loads[0] // sum(loads)))
    least = 1 if total - largest >= amount - 1 else 0
    counts, rest = [largest] + [least] * (amount - 1), total - largest - least * (amount - 1)
    while rest > 0:
        free = [i for i in range(1, amount) if counts[i] < largest] or [i for i in range(1, amount) if counts[i] < bound]
        whole, left = sum([loads[i] for i in free]), rest
        for i in free:
            addition = min(bound - counts[i], max(1, left * loads[i] // whole), rest)
            counts[i] = counts[i] + addition
            rest = rest - addition
    return np.array(counts)


def setup_inputs(seed: int = 0) -> dict:
    key_of = jax.random.split(jax.random.key(seed), 14)
    coarse_density = draw_coarse_density(jax.random.fold_in(key_of[13], 71), 0)
    coarse_emission = jnp.clip(4.0 * jax.random.uniform(key_of[1], (CB * BROWS, 128), jnp.float32) ** steps_of(key_of[1], (CB * BROWS, 128), ((0, 8),), -0.2, 0.2), 0.0, 4.0)
    fine_density = draw_fine_density(jax.random.fold_in(key_of[13], 71), 0)
    fine_emission = jnp.clip(4.0 * jax.random.uniform(key_of[3], (FINE * BROWS, 128), jnp.float32) ** steps_of(key_of[3], (FINE * BROWS, 128), ((0, 32),), -0.2, 0.2), 0.0, 4.0)
    coarse_brick = touch_ends(jax.random.randint(key_of[4], (SLABSEG,), 0, CB), jax.random.fold_in(key_of[4], 1), 0, CB - 1).astype(jnp.int32)
    coarse_lane = touch_ends(jax.random.randint(key_of[5], (SLABSEG,), 0, BRICK * BRICK), jax.random.fold_in(key_of[5], 1), 0, (BRICK * BRICK) - 1).astype(jnp.int32)
    coarse_entry = draw_coarse_entry(jax.random.fold_in(key_of[13], 71), 0)
    coarse_count = draw_coarse_count(jax.random.fold_in(key_of[13], 71), 0)
    fine_owner_keys = jax.random.split(jax.random.fold_in(key_of[8], 1), SEGT // (GROUP_PIX * FSEG))
    fine_owner_turns = jax.random.permutation(jax.random.fold_in(key_of[8], 3), SEGT // (GROUP_PIX * FSEG))
    fine_owner = jax.vmap(lambda own, number: routed_block(jax.random.fold_in(key_of[8], 2), own, number, GROUP_PIX * FSEG, N_MORTON * N_LEVEL, 1, RCAP, 2))(fine_owner_keys, fine_owner_turns).reshape((SEGT, 1))
    fine_brick = touch_ends(jax.random.randint(key_of[9], (SEGT,), 0, FB), jax.random.fold_in(key_of[9], 1), 0, FB - 1).astype(jnp.int32)
    fine_lane = touch_ends(jax.random.randint(key_of[10], (SEGT,), 0, BRICK * BRICK), jax.random.fold_in(key_of[10], 1), 0, (BRICK * BRICK) - 1).astype(jnp.int32)
    fine_entry = draw_fine_entry(jax.random.fold_in(key_of[13], 71), 0)
    fine_count = draw_fine_count(jax.random.fold_in(key_of[13], 71), 0)
    return {"coarse_density": coarse_density, "coarse_emission": coarse_emission, "fine_density": fine_density, "fine_emission": fine_emission, "coarse_brick": coarse_brick, "coarse_lane": coarse_lane, "coarse_entry": coarse_entry, "coarse_count": coarse_count, "fine_owner": fine_owner, "fine_brick": fine_brick, "fine_lane": fine_lane, "fine_entry": fine_entry, "fine_count": fine_count}


def march(density_rows, emission_rows, lane_ids, entry_ids, count_ids):
    per_row = 128 // BRICK
    chosen = ((lane_ids % per_row)[:, None] == lax.broadcasted_iota(jnp.int32, (1, per_row), 1))[:, :, None]
    nothing = jnp.float32(0.0)
    dens_lane = jnp.sum(jnp.where(chosen, density_rows.reshape(-1, per_row, BRICK), nothing), axis=1).T
    emis_lane = jnp.sum(jnp.where(chosen, emission_rows.reshape(-1, per_row, BRICK), nothing), axis=1).T
    step_ids = lax.broadcasted_iota(jnp.int32, (BRICK, 1), 0)
    inside = (step_ids >= entry_ids[None, :]) & (step_ids < (entry_ids + count_ids)[None, :])
    optical = jnp.where(inside, dens_lane, nothing)
    before = jnp.cumsum(optical, axis=0) - optical
    opacity = 1.0 - jnp.exp(-optical)
    colors = jnp.sum(jnp.exp(-before) * opacity * emis_lane, axis=0)
    return colors, jnp.sum(optical, axis=0)


def sample_table(dens_table, emis_table, brick_ids, lane_ids, entry_ids, count_ids):
    row_index = brick_ids * BROWS + lane_ids // (128 // BRICK)
    return march(dens_table[row_index], emis_table[row_index], lane_ids, entry_ids, count_ids)


def reference(coarse_density, coarse_emission, fine_density, fine_emission, coarse_brick, coarse_lane, coarse_entry, coarse_count, fine_owner, fine_brick, fine_lane, fine_entry, fine_count):
    groups = N_MORTON * N_LEVEL
    owner = fine_owner[:, 0]

    def one_slab(inputs):
        c_brick, c_lane, c_entry, c_count, f_owner, f_brick, f_lane, f_entry, f_count = inputs
        coarse_color, coarse_depth = sample_table(coarse_density, coarse_emission, c_brick, c_lane, c_entry, c_count)
        global_brick = f_owner * FB + f_brick
        seg_color, seg_depth = sample_table(fine_density, fine_emission, global_brick, f_lane, f_entry, f_count)
        seg_color = seg_color.reshape(GROUP_PIX, FSEG)
        seg_depth = seg_depth.reshape(GROUP_PIX, FSEG)
        earlier = jnp.cumsum(seg_depth, axis=1) - seg_depth
        slab_color = coarse_color + jnp.exp(-coarse_depth) * jnp.sum(jnp.exp(-earlier) * seg_color, axis=1)
        slab_depth = coarse_depth + jnp.sum(seg_depth, axis=1)
        return slab_color, slab_depth

    inputs = (coarse_brick.reshape(groups, GROUP_PIX), coarse_lane.reshape(groups, GROUP_PIX), coarse_entry.reshape(groups, GROUP_PIX), coarse_count.reshape(groups, GROUP_PIX), owner.reshape(groups, GROUP_PIX * FSEG), fine_brick.reshape(groups, GROUP_PIX * FSEG), fine_lane.reshape(groups, GROUP_PIX * FSEG), fine_entry.reshape(groups, GROUP_PIX * FSEG), fine_count.reshape(groups, GROUP_PIX * FSEG))
    slab_color, slab_depth = lax.map(one_slab, inputs)
    slab_color = slab_color.reshape(N_MORTON, N_LEVEL, GROUP_PIX)
    slab_depth = slab_depth.reshape(N_MORTON, N_LEVEL, GROUP_PIX)
    earlier = jnp.cumsum(slab_depth, axis=1) - slab_depth
    image_color = jnp.sum(jnp.exp(-earlier) * slab_color, axis=1).reshape(N_MORTON * GROUP_PIX)
    transmittance = jnp.exp(-jnp.sum(slab_depth, axis=1)).reshape(N_MORTON * GROUP_PIX)
    return image_color, transmittance
```

```python
import functools

import jax
import jax.numpy as jnp
from jax import lax
from jax.experimental import pallas as pl
from jax.experimental.pallas import tpu as pltpu
from jax.sharding import PartitionSpec as P

BRICK = 32
LANES = 128
SUBS = 8
PER_ROW = LANES // BRICK
COLUMNS = BRICK**2
F32 = jnp.float32
BF16 = jnp.bfloat16
I32 = jnp.int32
VMEM = pl.BlockSpec(memory_space=pltpu.VMEM)
ANY = pl.BlockSpec(memory_space=pl.ANY)


def iota(shape, dim):
    return lax.broadcasted_iota(I32, shape, dim)


def onehot(ids, width):
    return jnp.where(iota((width, ids.shape[1]), 0) == ids, 1.0, 0.0).astype(F32)


def split(x, parts):
    out = []
    for _ in range(parts):
        piece = x.astype(BF16)
        out.append(piece)
        x = x - piece.astype(F32)
    return out


def dot_nt(a, b):
    return lax.dot_general(a, b, (((1,), (1,)), ((), ())), preferred_element_type=F32)


def dot_nn(a, b):
    return jnp.dot(a, b, preferred_element_type=F32)


def across(ref, at, rows):
    return jnp.concatenate([ref[at + r : at + r + 1, :] for r in range(rows)], axis=1)


def rank_rows(ids_ref, width, ones_ref, within_ref, out_ref):
    rows = ids_ref.shape[0]
    for r in range(rows):
        ones_ref[r * width : (r + 1) * width, :] = onehot(ids_ref[r : r + 1, :], width).astype(BF16)
    lane, other = iota((LANES, 2 * LANES), 0), iota((LANES, 2 * LANES), 1)
    counter = jnp.where((lane < other) | (other >= LANES), 1.0, 0.0).astype(BF16)
    used = rows * width
    within_ref[:used, :] = dot_nn(ones_ref[:used, :], counter)
    ids_of = iota((width, LANES), 0)
    carry = jnp.zeros((width, LANES), F32)
    for r in range(rows):
        part = within_ref[r * width : (r + 1) * width, :]
        mine = jnp.where(ids_of == ids_ref[r : r + 1, :], part[:, :LANES] + carry, 0.0)
        out_ref[r : r + 1, :] = jnp.sum(mine, axis=0, keepdims=True).astype(I32)
        carry = carry + part[:, LANES:]


def place(cell_ref, lane_ref, code_ref, cells, chunk):
    rows = cell_ref.shape[0]
    placed = jnp.zeros((3 * cells, LANES), F32)
    for r in range(0, rows, chunk):
        here = iota((cells, chunk * LANES), 0) == across(cell_ref, r, chunk)
        code = across(code_ref, r, chunk)
        pieces = [code & 255, (code >> 8) & 255, code >> 16]
        left = jnp.concatenate([jnp.where(here, p.astype(F32), 0.0).astype(BF16) for p in pieces], axis=0)
        right = onehot(across(lane_ref, r, chunk), LANES).astype(BF16)
        placed = placed + dot_nt(left, right)
    a, b, c = (placed[i * cells : (i + 1) * cells].astype(I32) for i in range(3))
    return a + (b << 8) + (c << 16)


def cells_of(shape):
    rows = iota(shape, 0)
    return (rows & -BRICK) + 4 * (rows & 7) + ((rows >> 3) & 3)


def turn_tables(pairs):
    turn = jnp.where(cells_of((LANES, LANES)) == iota((LANES, LANES), 1), 1.0, 0.0).astype(BF16)
    for table_ref, dens_ref, emis_ref in pairs:
        for at, ref in ((0, dens_ref), (LANES, emis_ref)):
            for i, piece in enumerate(split(ref[...], 2)):
                top = 2 * LANES * i + at
                table_ref[top : top + LANES, :] = dot_nt(turn, piece).astype(BF16)


def fetch(codes, table_ref, got_ref):
    ones = onehot(codes >> 13, table_ref.shape[1]).astype(BF16)
    both = dot_nn(table_ref[...], ones)
    got_ref[...] = both[: 2 * LANES] + both[2 * LANES :]


def march(codes, got_ref, at):
    first = (codes >> 6) & 127
    last = first + (codes & 63)
    cells = cells_of((LANES, LANES))
    inside = (cells >= first) & (cells < last)
    dens = jnp.where(inside, got_ref[:LANES, at : at + LANES], 0.0)
    emis = jnp.where(inside, got_ref[LANES:, at : at + LANES], 0.0)
    dens = sum(dens[g * BRICK : (g + 1) * BRICK] for g in range(PER_ROW))
    emis = sum(emis[g * BRICK : (g + 1) * BRICK] for g in range(PER_ROW))
    trans = jnp.exp(-dens)
    color = (1.0 - trans) * emis
    c, t = color[24:32], trans[24:32]
    for k in (2, 1, 0):
        tk = trans[8 * k : 8 * k + 8]
        c = color[8 * k : 8 * k + 8] + tk * c
        t = tk * t
    for shift in (1, 2, 4):
        c = c + t * pltpu.roll(c, 8 - shift, 0)
        t = t * pltpu.roll(t, 8 - shift, 0)
    return c[0:1], t[0:1]


def look_up(resp_ref, at, blocks, width, cell_ref, lane_ref, left_ref, out_refs):
    n_dev, half = resp_ref.shape[0], resp_ref.shape[1] // 2
    high = blocks // width
    cells = high * n_dev
    for v in range(2):
        for h in range(high):
            for w in range(width):
                full = resp_ref[:, v * half + at + h * width + w, :]
                for i, piece in enumerate(split(full, 2)):
                    top = (2 * v + i) * cells + h * n_dev
                    left_ref[top : top + n_dev, w * LANES : (w + 1) * LANES] = piece
    rows = cell_ref.shape[0]
    chunk = SUBS
    left = left_ref[: 4 * cells, : width * LANES]
    for r in range(0, rows, chunk):
        got = dot_nn(left, onehot(across(lane_ref, r, chunk), width * LANES).astype(BF16))
        here = iota((cells, chunk * LANES), 0) == across(cell_ref, r, chunk)
        for v in range(2):
            total = got[2 * v * cells : (2 * v + 1) * cells] + got[(2 * v + 1) * cells : (2 * v + 2) * cells]
            value = jnp.sum(jnp.where(here, total, 0.0), axis=0, keepdims=True)
            for j in range(chunk):
                out_refs[v][r + j : r + j + 1, :] = value[:, j * LANES : (j + 1) * LANES]


def lanes_at(x, lanes):
    return jnp.take_along_axis(x, lanes, axis=1)


def blend(per_pixel, fine_c, fine_t, coarse_c, coarse_t, slab_ref):
    rows = fine_c.shape[0]
    level_rows = slab_ref.shape[1] // 2
    pixel_lanes = LANES // per_pixel
    lane = iota((SUBS, LANES), 1)
    source = (lane & (pixel_lanes - 1)) * per_pixel
    group = lane // pixel_lanes
    for r in range(0, rows, SUBS):
        c, t = fine_c[r : r + SUBS, :], fine_t[r : r + SUBS, :]
        shift = 1
        while shift < per_pixel:
            c = c + t * pltpu.roll(c, LANES - shift, 1)
            t = t * pltpu.roll(t, LANES - shift, 1)
            shift *= 2
        c, t = lanes_at(c, source), lanes_at(t, source)
        c, t = jnp.take_along_axis(c, group, axis=0)[0:1], jnp.take_along_axis(t, group, axis=0)[0:1]
        row = r // SUBS
        c0, t0 = coarse_c[row : row + 1, :], coarse_t[row : row + 1, :]
        to, at = row // level_rows, row % level_rows
        slab_ref[to, at : at + 1, :] = c0 + t0 * c
        slab_ref[to, level_rows + at : level_rows + at + 1, :] = t0 * t


def frame_kernel(n_morton, n_level, cap_f, cap_c, *refs):
    ints, tables, (color_ref, trans_ref), refs = refs[:9], refs[9:13], refs[13:15], refs[15:]
    int_refs, table_refs, refs = refs[:9], refs[9:13], refs[13:]
    (
        owner_ref,
        fcode_ref,
        frank_ref,
        fcell_ref,
        flane_ref,
        group_ref,
        ccode_ref,
        crank_ref,
        ccell_ref,
        clane_ref,
        ones_ref,
        within_ref,
        ft_ref,
        ct_ref,
        left_ref,
        fc_ref,
        ftr_ref,
        cc_ref,
        ctr_ref,
        msg_ref,
        code_ref,
        served_ref,
        resp_ref,
        slab_ref,
        slabs_ref,
        ask_send,
        ask_recv,
        tell_send,
        tell_recv,
        join_send,
        join_recv,
        in_sems,
        *refs,
    ) = refs
    even, odd = refs[:2], refs[2:]
    n_dev = n_morton * n_level
    nf, nc = cap_f // LANES, cap_c // LANES
    blocks = nf + nc
    copies = [
        pltpu.make_async_copy(src, dst, in_sems.at[i])
        for i, (src, dst) in enumerate(zip(ints + tables, int_refs + table_refs))
    ]
    for copy in copies[:9]:
        copy.start()
    morton, level = lax.axis_index("morton"), lax.axis_index("level")
    me = morton * n_level + level
    mesh_ids = pl.DeviceIdType.MESH

    def device(d):
        return d // n_level, lax.rem(d, n_level)

    def after(k):
        return lax.rem(me + k, n_dev)

    def before(k):
        return lax.rem(me + n_dev - k, n_dev)

    def ask(k):
        to = after(k)
        return pltpu.make_async_remote_copy(
            src_ref=msg_ref.at[to],
            dst_ref=code_ref.at[me],
            send_sem=ask_send.at[k],
            recv_sem=ask_recv.at[k],
            device_id=device(to),
            device_id_type=mesh_ids,
        )

    def tell(k):
        to = before(k)
        return pltpu.make_async_remote_copy(
            src_ref=served_ref.at[to],
            dst_ref=resp_ref.at[me],
            send_sem=tell_send.at[k],
            recv_sem=tell_recv.at[k],
            device_id=device(to),
            device_id_type=mesh_ids,
        )

    def join(k):
        to = lax.rem(level + k, n_level)
        return pltpu.make_async_remote_copy(
            src_ref=slab_ref.at[to],
            dst_ref=slabs_ref.at[level],
            send_sem=join_send.at[k],
            recv_sem=join_recv.at[k],
            device_id=(morton, to),
            device_id_type=mesh_ids,
        )

    barrier = pltpu.get_barrier_semaphore()

    def each(low, high, act):
        def body(k, _):
            act(k)
            return 0

        lax.fori_loop(low, high, body, 0)

    each(1, n_dev, lambda k: pl.semaphore_signal(barrier, inc=1, device_id=device(after(k)), device_id_type=mesh_ids))
    for copy in copies[9:]:
        copy.start()
    for copy in copies[:9]:
        copy.wait()
    f_owner, f_brick, f_lane, f_entry, f_count, c_brick, c_lane, c_entry, c_count = int_refs

    owner_ref[...] = f_owner[...]
    fcode_ref[...] = (((f_brick[...] * COLUMNS + f_lane[...]) * BRICK + f_entry[...]) << 6) + f_count[...]
    rank_rows(owner_ref, n_dev, ones_ref, within_ref, frank_ref)
    rank = frank_ref[...]
    fcell_ref[...] = f_owner[...] * nf + rank // LANES
    flane_ref[...] = rank & (LANES - 1)
    fine_msg = place(fcell_ref, flane_ref, fcode_ref, n_dev * nf, SUBS)

    c_cols = table_refs[2].shape[0] * PER_ROW
    column = c_brick[...] * COLUMNS + c_lane[...]
    group_ref[...] = column // c_cols
    ccode_ref[...] = (((column & (c_cols - 1)) * BRICK + c_entry[...]) << 6) + c_count[...]
    rank_rows(group_ref, n_morton, ones_ref, within_ref, crank_ref)
    rank = crank_ref[...]
    slot = rank // n_level
    dest = group_ref[...] * n_level + (rank & (n_level - 1))
    ccell_ref[...] = dest * nc + slot // LANES
    clane_ref[...] = slot & (LANES - 1)
    coarse_msg = place(ccell_ref, clane_ref, ccode_ref, n_dev * nc, SUBS)
    for i in range(n_dev):
        msg_ref[i, :nf, :] = fine_msg[i * nf : (i + 1) * nf]
        msg_ref[i, nf:, :] = coarse_msg[i * nc : (i + 1) * nc]

    pl.semaphore_wait(barrier, n_dev - 1)
    each(1, n_dev, lambda k: ask(k).start())
    code_ref[me] = msg_ref[me]
    for copy in copies[9:]:
        copy.wait()
    fd_ref, fe_ref, cd_ref, ce_ref = table_refs
    turn_tables(((ft_ref, fd_ref, fe_ref), (ct_ref, cd_ref, ce_ref)))

    def codes_of(i, at, rows):
        return jnp.concatenate([code_ref[i, at + r : at + r + 1, :] for r in range(rows)], axis=1)

    def fetch_source(i, bufs):
        fetch(codes_of(i, 0, nf), ft_ref, bufs[0])
        fetch(codes_of(i, nf, nc), ct_ref, bufs[1])

    def march_source(i, bufs):
        for b in range(blocks):
            buf, at = (bufs[0], b) if b < nf else (bufs[1], b - nf)
            c, t = march(code_ref[i, b : b + 1, :], buf, at * LANES)
            served_ref[i, b : b + 1, :] = c
            served_ref[i, blocks + b : blocks + b + 1, :] = t

    for ref in odd:
        ref[...] = jnp.zeros(ref.shape, F32)

    def two_sources(j, _):
        for u in range(2):

            @pl.when(2 * j + u > 0)
            def _():
                ask(2 * j + u).wait_recv()

            @pl.when(2 * j - 3 + u > 0)
            def _():
                tell(2 * j - 3 + u).start()

        now, later = before(2 * j), before(2 * j + 1)
        fetch_source(now, even)
        march_source(before(jnp.maximum(2 * j - 1, 0)), odd)
        fetch_source(later, odd)
        march_source(now, even)
        return 0

    lax.fori_loop(0, n_dev // 2, two_sources, 0)
    for k in (n_dev - 3, n_dev - 2):
        if k > 0:
            tell(k).start()
    march_source(before(n_dev - 1), odd)
    tell(n_dev - 1).start()
    resp_ref[me] = served_ref[me]
    rank = frank_ref[...]
    wf, wc = min(nf, 2), min(nc, 2)
    fcell_ref[...] = owner_ref[...] + (rank // (wf * LANES)) * n_dev
    flane_ref[...] = rank & (wf * LANES - 1)
    rank = crank_ref[...]
    slot = rank // n_level
    ccell_ref[...] = group_ref[...] * n_level + (rank & (n_level - 1)) + (slot // (wc * LANES)) * n_dev
    clane_ref[...] = slot & (wc * LANES - 1)
    each(1, n_dev, lambda k: tell(k).wait_recv())
    look_up(resp_ref, nf, nc, wc, ccell_ref, clane_ref, left_ref, (cc_ref, ctr_ref))
    look_up(resp_ref, 0, nf, wf, fcell_ref, flane_ref, left_ref, (fc_ref, ftr_ref))
    blend(owner_ref.shape[0] // group_ref.shape[0], fc_ref, ftr_ref, cc_ref, ctr_ref, slab_ref)
    for k in range(1, n_level):
        join(k).start()
    slabs_ref[level] = slab_ref[level]
    each(1, n_dev, lambda k: ask(k).wait_send())
    each(1, n_dev, lambda k: tell(k).wait_send())
    for k in range(1, n_level):
        join(k).wait()
    rows = color_ref.shape[0]
    color, trans = slabs_ref[0, :rows, :], slabs_ref[0, rows:, :]
    for s in range(1, n_level):
        color = color + trans * slabs_ref[s, :rows, :]
        trans = trans * slabs_ref[s, rows:, :]
    color_ref[...] = color
    trans_ref[...] = trans


def shards(
    coarse_density,
    coarse_emission,
    fine_density,
    fine_emission,
    coarse_brick,
    coarse_lane,
    coarse_entry,
    coarse_count,
    fine_owner,
    fine_brick,
    fine_lane,
    fine_entry,
    fine_count,
):
    n_morton = lax.axis_size("morton")
    n_level = lax.axis_size("level")
    n_dev = n_morton * n_level
    segments = fine_brick.shape[0]
    pixels = coarse_brick.shape[0]
    cap_f = -(-(2 * segments // n_dev) // LANES) * LANES
    cap_c = -(-pixels // (n_level * LANES)) * LANES
    nf, nc = cap_f // LANES, cap_c // LANES
    blocks = nf + nc
    f_rows, c_rows = segments // LANES, pixels // LANES
    level_rows = c_rows // n_level
    ints = [x.reshape(f_rows, LANES) for x in (fine_owner, fine_brick, fine_lane, fine_entry, fine_count)]
    ints += [x.reshape(c_rows, LANES) for x in (coarse_brick, coarse_lane, coarse_entry, coarse_count)]
    tables = [fine_density, fine_emission, coarse_density, coarse_emission]
    t_rows, g_rows = fine_density.shape[0], coarse_density.shape[0]
    wide = max(f_rows * n_dev, c_rows * n_morton)
    left_rows = 4 * n_dev * max(nf // min(nf, 2), nc // min(nc, 2))

    def like(x):
        return pltpu.VMEM(x.shape, x.dtype)

    sems = [pltpu.SemaphoreType.DMA((n_dev,))] * 4 + [pltpu.SemaphoreType.DMA((n_level,))] * 2
    color, trans = pl.pallas_call(
        functools.partial(frame_kernel, n_morton, n_level, cap_f, cap_c),
        out_shape=[jax.ShapeDtypeStruct((level_rows, LANES), F32)] * 2,
        in_specs=[ANY] * 13,
        out_specs=[VMEM] * 2,
        scratch_shapes=[like(x) for x in ints + tables]
        + [pltpu.VMEM((f_rows, LANES), I32)] * 5
        + [pltpu.VMEM((c_rows, LANES), I32)] * 5
        + [
            pltpu.VMEM((wide, LANES), BF16),
            pltpu.VMEM((wide, 2 * LANES), F32),
            pltpu.VMEM((4 * LANES, t_rows), BF16),
            pltpu.VMEM((4 * LANES, g_rows), BF16),
            pltpu.VMEM((left_rows, 2 * LANES), BF16),
        ]
        + [pltpu.VMEM((f_rows, LANES), F32)] * 2
        + [pltpu.VMEM((c_rows, LANES), F32)] * 2
        + [
            pltpu.VMEM((n_dev, blocks, LANES), I32),
            pltpu.VMEM((n_dev, blocks, LANES), I32),
            pltpu.VMEM((n_dev, 2 * blocks, LANES), F32),
            pltpu.VMEM((n_dev, 2 * blocks, LANES), F32),
            pltpu.VMEM((n_level, 2 * level_rows, LANES), F32),
            pltpu.VMEM((n_level, 2 * level_rows, LANES), F32),
        ]
        + sems
        + [pltpu.SemaphoreType.DMA((13,))]
        + [pltpu.VMEM((2 * LANES, cap_f), F32), pltpu.VMEM((2 * LANES, cap_c), F32)] * 2,
        compiler_params=pltpu.CompilerParams(collective_id=0, has_side_effects=True),
    )(*ints, *tables)
    return color.reshape(-1), trans.reshape(-1)


def solution(mesh):
    both = P(("morton", "level"))
    rows = P(("morton", "level"), None)
    coarse = P("morton", None)
    return jax.shard_map(
        shards,
        mesh=mesh,
        in_specs=(coarse, coarse, rows, rows, both, both, both, both, rows, both, both, both, both),
        out_specs=(both, both),
        check_vma=False,
    )
```

```python
import functools

import jax
import jax.numpy as jnp
from jax import lax
from jax.experimental import pallas as pl
from jax.experimental.pallas import tpu as pltpu
from jax.sharding import PartitionSpec as P

BRICK = 32
LANES = 128
SUBS = 8
PER_ROW = LANES // BRICK
COLUMNS = BRICK**2
F32 = jnp.float32
BF16 = jnp.bfloat16
I32 = jnp.int32
VMEM = pl.BlockSpec(memory_space=pltpu.VMEM)
ANY = pl.BlockSpec(memory_space=pl.ANY)


def iota(shape, dim):
    return lax.broadcasted_iota(I32, shape, dim)


def onehot(ids, width):
    return jnp.where(iota((width, ids.shape[1]), 0) == ids, 1.0, 0.0).astype(F32)


def split(x, parts):
    out = []
    for _ in range(parts):
        piece = x.astype(BF16)
        out.append(piece)
        x = x - piece.astype(F32)
    return out


def dot_nt(a, b):
    return lax.dot_general(a, b, (((1,), (1,)), ((), ())), preferred_element_type=F32)


def dot_nn(a, b):
    return jnp.dot(a, b, preferred_element_type=F32)


def across(ref, at, rows):
    return jnp.concatenate([ref[at + r : at + r + 1, :] for r in range(rows)], axis=1)


def rank_rows(ids_ref, width, ones_ref, within_ref, out_ref):
    rows = ids_ref.shape[0]
    for r in range(rows):
        ones_ref[r * width : (r + 1) * width, :] = onehot(ids_ref[r : r + 1, :], width).astype(BF16)
    lane, other = iota((LANES, 2 * LANES), 0), iota((LANES, 2 * LANES), 1)
    counter = jnp.where((lane < other) | (other >= LANES), 1.0, 0.0).astype(BF16)
    used = rows * width
    within_ref[:used, :] = dot_nn(ones_ref[:used, :], counter)
    ids_of = iota((width, LANES), 0)
    carry = jnp.zeros((width, LANES), F32)
    for r in range(rows):
        part = within_ref[r * width : (r + 1) * width, :]
        mine = jnp.where(ids_of == ids_ref[r : r + 1, :], part[:, :LANES] + carry, 0.0)
        out_ref[r : r + 1, :] = jnp.sum(mine, axis=0, keepdims=True).astype(I32)
        carry = carry + part[:, LANES:]


def place(cell_ref, lane_ref, code_ref, cells, chunk):
    rows = cell_ref.shape[0]
    placed = jnp.zeros((3 * cells, LANES), F32)
    for r in range(0, rows, chunk):
        here = iota((cells, chunk * LANES), 0) == across(cell_ref, r, chunk)
        code = across(code_ref, r, chunk)
        pieces = [code & 255, (code >> 8) & 255, code >> 16]
        left = jnp.concatenate([jnp.where(here, p.astype(F32), 0.0).astype(BF16) for p in pieces], axis=0)
        right = onehot(across(lane_ref, r, chunk), LANES).astype(BF16)
        placed = placed + dot_nt(left, right)
    a, b, c = (placed[i * cells : (i + 1) * cells].astype(I32) for i in range(3))
    return a + (b << 8) + (c << 16)


def cells_of(shape):
    rows = iota(shape, 0)
    return (rows & -BRICK) + 4 * (rows & 7) + ((rows >> 3) & 3)


def turned(turn, ref, parts):
    return [dot_nt(turn, piece) for piece in split(ref[...], parts)]


def turn_tables(ft_ref, fd_ref, fe_ref, ct_ref, cd_ref, ce_ref):
    turn = jnp.where(cells_of((LANES, LANES)) == iota((LANES, LANES), 1), 1.0, 0.0).astype(BF16)
    for at, ref in ((0, fd_ref), (LANES, fe_ref)):
        for i, piece in enumerate(turned(turn, ref, 2)):
            top = 2 * LANES * i + at
            ft_ref[top : top + LANES, :] = piece.astype(BF16)
    wide = ct_ref.shape[0] // PER_ROW
    rows = cd_ref.shape[0]
    for v, ref in enumerate((cd_ref, ce_ref)):
        whole = sum(turned(turn, ref, 3))
        for q in range(PER_ROW):
            for at in range(0, rows, LANES):
                size = min(LANES, rows - at)
                top = q * wide + (at // LANES) * 2 * BRICK + v * BRICK
                ct_ref[top : top + BRICK, :size] = whole[q * BRICK : (q + 1) * BRICK, at : at + size]


def fetch(codes, table_ref, got_ref):
    ones = onehot(codes >> 13, table_ref.shape[1]).astype(BF16)
    both = dot_nn(table_ref[...], ones)
    got_ref[...] = both[: 2 * LANES] + both[2 * LANES :]


def lanes_at(x, lanes):
    return jnp.take_along_axis(x, lanes, axis=1)


def front_to_back(dens, emis):
    trans = [jnp.exp(-d) for d in dens]
    color = [(1.0 - t) * e for t, e in zip(trans, emis)]
    c, t = color[3], trans[3]
    for k in (2, 1, 0):
        c = color[k] + trans[k] * c
        t = trans[k] * t
    for shift in (1, 2, 4):
        c = c + t * pltpu.roll(c, SUBS - shift, 0)
        t = t * pltpu.roll(t, SUBS - shift, 0)
    return c[0:1], t[0:1]


def march(codes, got_ref, at):
    first = (codes >> 6) & 127
    last = first + (codes & 63)
    cells = cells_of((LANES, LANES))
    inside = (cells >= first) & (cells < last)
    dens = jnp.where(inside, got_ref[:LANES, at : at + LANES], 0.0)
    emis = jnp.where(inside, got_ref[LANES:, at : at + LANES], 0.0)
    dens = sum(dens[g * BRICK : (g + 1) * BRICK] for g in range(PER_ROW))
    emis = sum(emis[g * BRICK : (g + 1) * BRICK] for g in range(PER_ROW))
    steps = range(0, BRICK, SUBS)
    return front_to_back([dens[k : k + SUBS] for k in steps], [emis[k : k + SUBS] for k in steps])


def march_lanes(codes, table_ref):
    codes = jnp.broadcast_to(codes, (SUBS, LANES))
    row = codes >> 13
    wide = table_ref.shape[0] // (PER_ROW * 2 * BRICK)
    group = ((codes >> 11) & (PER_ROW - 1)) * wide + row // LANES
    lane = row & (LANES - 1)
    got = [None] * (2 * BRICK // SUBS)
    for g in range(PER_ROW * wide):
        here = group == g
        for v in range(len(got)):
            top = g * 2 * BRICK + v * SUBS
            value = lanes_at(table_ref[top : top + SUBS, :], lane)
            got[v] = value if g == 0 else jnp.where(here, value, got[v])
    first = (codes >> 6) & (BRICK - 1)
    last = first + (codes & 63)
    steps = BRICK // SUBS
    cells = [steps * iota((SUBS, LANES), 0) + k for k in range(steps)]
    inside = [(c >= first) & (c < last) for c in cells]
    dens = [jnp.where(m, x, 0.0) for m, x in zip(inside, got[:steps])]
    return front_to_back(dens, got[steps:])


def look_up(resp_ref, at, blocks, width, cell_ref, lane_ref, left_ref, out_refs):
    n_dev, half = resp_ref.shape[0], resp_ref.shape[1] // 2
    high = blocks // width
    cells = high * n_dev
    for v in range(2):
        for h in range(high):
            for w in range(width):
                full = resp_ref[:, v * half + at + h * width + w, :]
                for i, piece in enumerate(split(full, 2)):
                    top = (2 * v + i) * cells + h * n_dev
                    left_ref[top : top + n_dev, w * LANES : (w + 1) * LANES] = piece
    rows = cell_ref.shape[0]
    chunk = SUBS
    left = left_ref[: 4 * cells, : width * LANES]
    for r in range(0, rows, chunk):
        got = dot_nn(left, onehot(across(lane_ref, r, chunk), width * LANES).astype(BF16))
        here = iota((cells, chunk * LANES), 0) == across(cell_ref, r, chunk)
        for v in range(2):
            total = got[2 * v * cells : (2 * v + 1) * cells] + got[(2 * v + 1) * cells : (2 * v + 2) * cells]
            value = jnp.sum(jnp.where(here, total, 0.0), axis=0, keepdims=True)
            for j in range(chunk):
                out_refs[v][r + j : r + j + 1, :] = value[:, j * LANES : (j + 1) * LANES]


def blend(per_pixel, fine_c, fine_t, coarse_c, coarse_t, slab_ref):
    rows = fine_c.shape[0]
    level_rows = slab_ref.shape[1] // 2
    pixel_lanes = LANES // per_pixel
    lane = iota((SUBS, LANES), 1)
    source = (lane & (pixel_lanes - 1)) * per_pixel
    group = lane // pixel_lanes
    for r in range(0, rows, SUBS):
        c, t = fine_c[r : r + SUBS, :], fine_t[r : r + SUBS, :]
        shift = 1
        while shift < per_pixel:
            c = c + t * pltpu.roll(c, LANES - shift, 1)
            t = t * pltpu.roll(t, LANES - shift, 1)
            shift *= 2
        c, t = lanes_at(c, source), lanes_at(t, source)
        c, t = jnp.take_along_axis(c, group, axis=0)[0:1], jnp.take_along_axis(t, group, axis=0)[0:1]
        row = r // SUBS
        c0, t0 = coarse_c[row : row + 1, :], coarse_t[row : row + 1, :]
        to, at = row // level_rows, row % level_rows
        slab_ref[to, at : at + 1, :] = c0 + t0 * c
        slab_ref[to, level_rows + at : level_rows + at + 1, :] = t0 * t


def frame_kernel(n_morton, n_level, cap_f, cap_c, *refs):
    ints, tables, (color_ref, trans_ref), refs = refs[:9], refs[9:13], refs[13:15], refs[15:]
    int_refs, table_refs, refs = refs[:9], refs[9:13], refs[13:]
    (
        owner_ref,
        fcode_ref,
        frank_ref,
        fcell_ref,
        flane_ref,
        group_ref,
        ccode_ref,
        crank_ref,
        ccell_ref,
        clane_ref,
        ones_ref,
        within_ref,
        ft_ref,
        ct_ref,
        left_ref,
        fc_ref,
        ftr_ref,
        cc_ref,
        ctr_ref,
        msg_ref,
        code_ref,
        served_ref,
        resp_ref,
        slab_ref,
        slabs_ref,
        ask_send,
        ask_recv,
        tell_send,
        tell_recv,
        join_send,
        join_recv,
        in_sems,
        *refs,
    ) = refs
    even, odd = refs
    n_dev = n_morton * n_level
    nf, nc = cap_f // LANES, cap_c // LANES
    blocks = nf + nc
    copies = [
        pltpu.make_async_copy(src, dst, in_sems.at[i])
        for i, (src, dst) in enumerate(zip(ints + tables, int_refs + table_refs))
    ]
    for copy in copies[:9]:
        copy.start()
    morton, level = lax.axis_index("morton"), lax.axis_index("level")
    me = morton * n_level + level
    mesh_ids = pl.DeviceIdType.MESH

    def device(d):
        return d // n_level, lax.rem(d, n_level)

    def after(k):
        return lax.rem(me + k, n_dev)

    def before(k):
        return lax.rem(me + n_dev - k, n_dev)

    early = max(n_dev // 4, 1)
    late = n_dev - early
    is_early = me < early
    place_in = jnp.where(is_early, me, me - early)

    def source(t):
        one = lax.rem(me + t, early)
        other = early + lax.rem(place_in + late + early - t, late)
        return jnp.where(t == 0, me, jnp.where(t < early + jnp.where(is_early, 0, 1), one, other))

    def steps_back(t):
        return lax.rem(me + n_dev - source(t), n_dev)

    def ask(k):
        to = after(k)
        return pltpu.make_async_remote_copy(
            src_ref=msg_ref.at[to],
            dst_ref=code_ref.at[me],
            send_sem=ask_send.at[k],
            recv_sem=ask_recv.at[k],
            device_id=device(to),
            device_id_type=mesh_ids,
        )

    def tell(k):
        to = before(k)
        return pltpu.make_async_remote_copy(
            src_ref=served_ref.at[to],
            dst_ref=resp_ref.at[me],
            send_sem=tell_send.at[k],
            recv_sem=tell_recv.at[k],
            device_id=device(to),
            device_id_type=mesh_ids,
        )

    def join(k):
        to = lax.rem(level + k, n_level)
        return pltpu.make_async_remote_copy(
            src_ref=slab_ref.at[to],
            dst_ref=slabs_ref.at[level],
            send_sem=join_send.at[k],
            recv_sem=join_recv.at[k],
            device_id=(morton, to),
            device_id_type=mesh_ids,
        )

    barrier = pltpu.get_barrier_semaphore()

    def each(low, high, act):
        def body(k, _):
            act(k)
            return 0

        lax.fori_loop(low, high, body, 0)

    each(1, n_dev, lambda k: pl.semaphore_signal(barrier, inc=1, device_id=device(after(k)), device_id_type=mesh_ids))
    for copy in copies[9:]:
        copy.start()
    for copy in copies[:9]:
        copy.wait()
    f_owner, f_brick, f_lane, f_entry, f_count, c_brick, c_lane, c_entry, c_count = int_refs

    owner_ref[...] = f_owner[...]
    fcode_ref[...] = (((f_brick[...] * COLUMNS + f_lane[...]) * BRICK + f_entry[...]) << 6) + f_count[...]
    rank_rows(owner_ref, n_dev, ones_ref, within_ref, frank_ref)
    rank = frank_ref[...]
    fcell_ref[...] = f_owner[...] * nf + rank // LANES
    flane_ref[...] = rank & (LANES - 1)
    fine_msg = place(fcell_ref, flane_ref, fcode_ref, n_dev * nf, SUBS)

    c_cols = table_refs[2].shape[0] * PER_ROW
    column = c_brick[...] * COLUMNS + c_lane[...]
    group_ref[...] = column // c_cols
    ccode_ref[...] = (((column & (c_cols - 1)) * BRICK + c_entry[...]) << 6) + c_count[...]
    rank_rows(group_ref, n_morton, ones_ref, within_ref, crank_ref)
    rank = crank_ref[...]
    slot = rank // n_level
    dest = group_ref[...] * n_level + (rank & (n_level - 1))
    ccell_ref[...] = dest * nc + slot // LANES
    clane_ref[...] = slot & (LANES - 1)
    coarse_msg = place(ccell_ref, clane_ref, ccode_ref, n_dev * nc, SUBS)
    for i in range(n_dev):
        msg_ref[i, :nf, :] = fine_msg[i * nf : (i + 1) * nf]
        msg_ref[i, nf:, :] = coarse_msg[i * nc : (i + 1) * nc]

    pl.semaphore_wait(barrier, n_dev - 1)
    each(1, n_dev, lambda k: ask(k).start())
    code_ref[me] = msg_ref[me]
    for copy in copies[9:]:
        copy.wait()
    fd_ref, fe_ref, cd_ref, ce_ref = table_refs
    turn_tables(ft_ref, fd_ref, fe_ref, ct_ref, cd_ref, ce_ref)

    def codes_of(i, at, rows):
        return jnp.concatenate([code_ref[i, at + r : at + r + 1, :] for r in range(rows)], axis=1)

    def put(i, b, c, t):
        served_ref[i, b : b + 1, :] = c
        served_ref[i, blocks + b : blocks + b + 1, :] = t

    def fetch_source(i, buf):
        fetch(codes_of(i, 0, nf), ft_ref, buf)
        for b in range(nf, blocks):
            put(i, b, *march_lanes(code_ref[i, b : b + 1, :], ct_ref))

    def march_source(i, buf):
        for b in range(nf):
            put(i, b, *march(code_ref[i, b : b + 1, :], buf, b * LANES))

    odd[...] = jnp.zeros(odd.shape, F32)

    def two_sources(j, _):
        for u in range(2):

            @pl.when(2 * j + u > 0)
            def _():
                ask(steps_back(2 * j + u)).wait_recv()

            @pl.when(2 * j - 3 + u > 0)
            def _():
                tell(steps_back(2 * j - 3 + u)).start()

        now, later = source(2 * j), source(2 * j + 1)
        fetch_source(now, even)
        march_source(source(jnp.maximum(2 * j - 1, 0)), odd)
        fetch_source(later, odd)
        march_source(now, even)
        return 0

    lax.fori_loop(0, n_dev // 2, two_sources, 0)
    for k in (n_dev - 3, n_dev - 2):
        if k > 0:
            tell(steps_back(k)).start()
    march_source(source(n_dev - 1), odd)
    tell(steps_back(n_dev - 1)).start()
    resp_ref[me] = served_ref[me]
    rank = frank_ref[...]
    wf, wc = min(nf, 2), min(nc, 2)
    fcell_ref[...] = owner_ref[...] + (rank // (wf * LANES)) * n_dev
    flane_ref[...] = rank & (wf * LANES - 1)
    rank = crank_ref[...]
    slot = rank // n_level
    ccell_ref[...] = group_ref[...] * n_level + (rank & (n_level - 1)) + (slot // (wc * LANES)) * n_dev
    clane_ref[...] = slot & (wc * LANES - 1)
    each(1, n_dev, lambda k: tell(k).wait_recv())
    look_up(resp_ref, nf, nc, wc, ccell_ref, clane_ref, left_ref, (cc_ref, ctr_ref))
    look_up(resp_ref, 0, nf, wf, fcell_ref, flane_ref, left_ref, (fc_ref, ftr_ref))
    blend(owner_ref.shape[0] // group_ref.shape[0], fc_ref, ftr_ref, cc_ref, ctr_ref, slab_ref)
    for k in range(1, n_level):
        join(k).start()
    slabs_ref[level] = slab_ref[level]
    each(1, n_dev, lambda k: ask(k).wait_send())
    each(1, n_dev, lambda k: tell(k).wait_send())
    for k in range(1, n_level):
        join(k).wait()
    rows = color_ref.shape[0]
    color, trans = slabs_ref[0, :rows, :], slabs_ref[0, rows:, :]
    for s in range(1, n_level):
        color = color + trans * slabs_ref[s, :rows, :]
        trans = trans * slabs_ref[s, rows:, :]
    color_ref[...] = color
    trans_ref[...] = trans


def shards(
    coarse_density,
    coarse_emission,
    fine_density,
    fine_emission,
    coarse_brick,
    coarse_lane,
    coarse_entry,
    coarse_count,
    fine_owner,
    fine_brick,
    fine_lane,
    fine_entry,
    fine_count,
):
    n_morton = lax.axis_size("morton")
    n_level = lax.axis_size("level")
    n_dev = n_morton * n_level
    segments = fine_brick.shape[0]
    pixels = coarse_brick.shape[0]
    cap_f = -(-(2 * segments // n_dev) // LANES) * LANES
    cap_c = -(-pixels // (n_level * LANES)) * LANES
    nf, nc = cap_f // LANES, cap_c // LANES
    blocks = nf + nc
    f_rows, c_rows = segments // LANES, pixels // LANES
    level_rows = c_rows // n_level
    ints = [x.reshape(f_rows, LANES) for x in (fine_owner, fine_brick, fine_lane, fine_entry, fine_count)]
    ints += [x.reshape(c_rows, LANES) for x in (coarse_brick, coarse_lane, coarse_entry, coarse_count)]
    tables = [fine_density, fine_emission, coarse_density, coarse_emission]
    t_rows, g_rows = fine_density.shape[0], coarse_density.shape[0]
    wide = max(f_rows * n_dev, c_rows * n_morton)
    left_rows = 4 * n_dev * max(nf // min(nf, 2), nc // min(nc, 2))

    def like(x):
        return pltpu.VMEM(x.shape, x.dtype)

    sems = [pltpu.SemaphoreType.DMA((n_dev,))] * 4 + [pltpu.SemaphoreType.DMA((n_level,))] * 2
    color, trans = pl.pallas_call(
        functools.partial(frame_kernel, n_morton, n_level, cap_f, cap_c),
        out_shape=[jax.ShapeDtypeStruct((level_rows, LANES), F32)] * 2,
        in_specs=[ANY] * 13,
        out_specs=[VMEM] * 2,
        scratch_shapes=[like(x) for x in ints + tables]
        + [pltpu.VMEM((f_rows, LANES), I32)] * 5
        + [pltpu.VMEM((c_rows, LANES), I32)] * 5
        + [
            pltpu.VMEM((wide, LANES), BF16),
            pltpu.VMEM((wide, 2 * LANES), F32),
            pltpu.VMEM((4 * LANES, t_rows), BF16),
            pltpu.VMEM((-(-g_rows // LANES) * PER_ROW * 2 * BRICK, LANES), F32),
            pltpu.VMEM((left_rows, 2 * LANES), BF16),
        ]
        + [pltpu.VMEM((f_rows, LANES), F32)] * 2
        + [pltpu.VMEM((c_rows, LANES), F32)] * 2
        + [
            pltpu.VMEM((n_dev, blocks, LANES), I32),
            pltpu.VMEM((n_dev, blocks, LANES), I32),
            pltpu.VMEM((n_dev, 2 * blocks, LANES), F32),
            pltpu.VMEM((n_dev, 2 * blocks, LANES), F32),
            pltpu.VMEM((n_level, 2 * level_rows, LANES), F32),
            pltpu.VMEM((n_level, 2 * level_rows, LANES), F32),
        ]
        + sems
        + [pltpu.SemaphoreType.DMA((13,))]
        + [pltpu.VMEM((2 * LANES, cap_f), F32)] * 2,
        compiler_params=pltpu.CompilerParams(collective_id=0, has_side_effects=True),
    )(*ints, *tables)
    return color.reshape(-1), trans.reshape(-1)


def solution(mesh):
    both = P(("morton", "level"))
    rows = P(("morton", "level"), None)
    coarse = P("morton", None)
    return jax.shard_map(
        shards,
        mesh=mesh,
        in_specs=(coarse, coarse, rows, rows, both, both, both, both, rows, both, both, both, both),
        out_specs=(both, both),
        check_vma=False,
    )
```

```python
import functools

import jax
import jax.numpy as jnp
from jax import lax
from jax.experimental import pallas as pl
from jax.experimental.pallas import tpu as pltpu
from jax.sharding import PartitionSpec as P

BRICK = 32
LANES = 128
SUBS = 8
PER_ROW = LANES // BRICK
COLUMNS = BRICK**2
F32 = jnp.float32
BF16 = jnp.bfloat16
I32 = jnp.int32
VMEM = pl.BlockSpec(memory_space=pltpu.VMEM)
ANY = pl.BlockSpec(memory_space=pl.ANY)


def iota(shape, dim):
    return lax.broadcasted_iota(I32, shape, dim)


def onehot(ids, width):
    return jnp.where(iota((width, ids.shape[1]), 0) == ids, 1.0, 0.0).astype(F32)


def split(x, parts):
    out = []
    for _ in range(parts):
        piece = x.astype(BF16)
        out.append(piece)
        x = x - piece.astype(F32)
    return out


def dot_nt(a, b):
    return lax.dot_general(a, b, (((1,), (1,)), ((), ())), preferred_element_type=F32)


def dot_nn(a, b):
    return jnp.dot(a, b, preferred_element_type=F32)


def across(ref, at, rows):
    return jnp.concatenate([ref[at + r : at + r + 1, :] for r in range(rows)], axis=1)


def rank_rows(ids_ref, width, ones_ref, within_ref, out_ref):
    rows = ids_ref.shape[0]
    for r in range(rows):
        ones_ref[r * width : (r + 1) * width, :] = onehot(ids_ref[r : r + 1, :], width).astype(BF16)
    lane, other = iota((LANES, 2 * LANES), 0), iota((LANES, 2 * LANES), 1)
    counter = jnp.where((lane < other) | (other >= LANES), 1.0, 0.0).astype(BF16)
    used = rows * width
    within_ref[:used, :] = dot_nn(ones_ref[:used, :], counter)
    ids_of = iota((width, LANES), 0)
    carry = jnp.zeros((width, LANES), F32)
    for r in range(rows):
        part = within_ref[r * width : (r + 1) * width, :]
        mine = jnp.where(ids_of == ids_ref[r : r + 1, :], part[:, :LANES] + carry, 0.0)
        out_ref[r : r + 1, :] = jnp.sum(mine, axis=0, keepdims=True).astype(I32)
        carry = carry + part[:, LANES:]


def to_float(value):
    return ((LANES + (value & (LANES - 1))) << (value >> 7)).astype(F32)


def from_float(x):
    y = x.astype(I32)
    shift = jnp.zeros_like(y)
    for bits in (8, 4, 2, 1):
        over = y >= (LANES << bits)
        y = jnp.where(over, y >> bits, y)
        shift = jnp.where(over, shift + bits, shift)
    return jnp.where(y == 0, 0, y - LANES + (shift << 7))


def place(cell_ref, lane_ref, code_ref, cells, chunk):
    rows = cell_ref.shape[0]
    placed = jnp.zeros((2 * cells, LANES), F32)
    for r in range(0, rows, chunk):
        here = iota((cells, chunk * LANES), 0) == across(cell_ref, r, chunk)
        code = across(code_ref, r, chunk)
        pieces = [to_float(code >> 11), to_float(code & 2047)]
        left = jnp.concatenate([jnp.where(here, p, 0.0).astype(BF16) for p in pieces], axis=0)
        right = onehot(across(lane_ref, r, chunk), LANES).astype(BF16)
        placed = placed + dot_nt(left, right)
    return (from_float(placed[:cells]) << 11) + from_float(placed[cells:])


def cells_of(shape):
    rows = iota(shape, 0)
    return (rows & -BRICK) + 4 * (rows & 7) + ((rows >> 3) & 3)


def turned(turn, ref, parts):
    return [dot_nt(turn, piece) for piece in split(ref[...], parts)]


def turn_tables(ft_ref, fd_ref, fe_ref, ct_ref, cd_ref, ce_ref):
    turn = jnp.where(cells_of((LANES, LANES)) == iota((LANES, LANES), 1), 1.0, 0.0).astype(BF16)
    for at, ref in ((0, fd_ref), (LANES, fe_ref)):
        for i, piece in enumerate(turned(turn, ref, 2)):
            top = 2 * LANES * i + at
            ft_ref[top : top + LANES, :] = piece.astype(BF16)
    wide = ct_ref.shape[0] // PER_ROW
    rows = cd_ref.shape[0]
    for v, ref in enumerate((cd_ref, ce_ref)):
        whole = sum(turned(turn, ref, 3))
        for q in range(PER_ROW):
            for at in range(0, rows, LANES):
                size = min(LANES, rows - at)
                top = q * wide + (at // LANES) * 2 * BRICK + v * BRICK
                ct_ref[top : top + BRICK, :size] = whole[q * BRICK : (q + 1) * BRICK, at : at + size]


def fetch(codes, table_ref, got_ref):
    ones = onehot(codes >> 13, table_ref.shape[1]).astype(BF16)
    both = dot_nn(table_ref[...], ones)
    got_ref[...] = both[: 2 * LANES] + both[2 * LANES :]


def lanes_at(x, lanes):
    return jnp.take_along_axis(x, lanes, axis=1)


def front_to_back(dens, emis):
    trans = [jnp.exp(-d) for d in dens]
    color = [(1.0 - t) * e for t, e in zip(trans, emis)]
    c, t = color[3], trans[3]
    for k in (2, 1, 0):
        c = color[k] + trans[k] * c
        t = trans[k] * t
    for shift in (1, 2, 4):
        c = c + t * pltpu.roll(c, SUBS - shift, 0)
        t = t * pltpu.roll(t, SUBS - shift, 0)
    return c[0:1], t[0:1]


def march(codes, got_ref, at):
    first = (codes >> 6) & 127
    last = first + (codes & 63)
    cells = cells_of((LANES, LANES))
    inside = (cells >= first) & (cells < last)
    dens = jnp.where(inside, got_ref[:LANES, at : at + LANES], 0.0)
    emis = jnp.where(inside, got_ref[LANES:, at : at + LANES], 0.0)
    dens = sum(dens[g * BRICK : (g + 1) * BRICK] for g in range(PER_ROW))
    emis = sum(emis[g * BRICK : (g + 1) * BRICK] for g in range(PER_ROW))
    steps = range(0, BRICK, SUBS)
    return front_to_back([dens[k : k + SUBS] for k in steps], [emis[k : k + SUBS] for k in steps])


def march_lanes(codes, table_ref):
    codes = jnp.broadcast_to(codes, (SUBS, LANES))
    row = codes >> 13
    wide = table_ref.shape[0] // (PER_ROW * 2 * BRICK)
    group = ((codes >> 11) & (PER_ROW - 1)) * wide + row // LANES
    lane = row & (LANES - 1)
    got = [None] * (2 * BRICK // SUBS)
    for g in range(PER_ROW * wide):
        here = group == g
        for v in range(len(got)):
            top = g * 2 * BRICK + v * SUBS
            value = lanes_at(table_ref[top : top + SUBS, :], lane)
            got[v] = value if g == 0 else jnp.where(here, value, got[v])
    first = (codes >> 6) & (BRICK - 1)
    last = first + (codes & 63)
    steps = BRICK // SUBS
    cells = [steps * iota((SUBS, LANES), 0) + k for k in range(steps)]
    inside = [(c >= first) & (c < last) for c in cells]
    dens = [jnp.where(m, x, 0.0) for m, x in zip(inside, got[:steps])]
    return front_to_back(dens, got[steps:])


def look_up(resp_ref, at, blocks, width, cell_ref, lane_ref, left_ref, out_refs):
    n_dev, half = resp_ref.shape[0], resp_ref.shape[1] // 2
    high = blocks // width
    cells = high * n_dev
    for v in range(2):
        for h in range(high):
            for w in range(width):
                full = resp_ref[:, v * half + at + h * width + w, :]
                for i, piece in enumerate(split(full, 2)):
                    top = (2 * v + i) * cells + h * n_dev
                    left_ref[top : top + n_dev, w * LANES : (w + 1) * LANES] = piece
    rows = cell_ref.shape[0]
    chunk = SUBS
    left = left_ref[: 4 * cells, : width * LANES]
    for r in range(0, rows, chunk):
        got = dot_nn(left, onehot(across(lane_ref, r, chunk), width * LANES).astype(BF16))
        here = iota((cells, chunk * LANES), 0) == across(cell_ref, r, chunk)
        for v in range(2):
            total = got[2 * v * cells : (2 * v + 1) * cells] + got[(2 * v + 1) * cells : (2 * v + 2) * cells]
            value = jnp.sum(jnp.where(here, total, 0.0), axis=0, keepdims=True)
            for j in range(chunk):
                out_refs[v][r + j : r + j + 1, :] = value[:, j * LANES : (j + 1) * LANES]


def blend(per_pixel, fine_c, fine_t, coarse_c, coarse_t, slab_ref):
    rows = fine_c.shape[0]
    level_rows = slab_ref.shape[1] // 2
    pixel_lanes = LANES // per_pixel
    lane = iota((SUBS, LANES), 1)
    source = (lane & (pixel_lanes - 1)) * per_pixel
    group = lane // pixel_lanes
    for r in range(0, rows, SUBS):
        c, t = fine_c[r : r + SUBS, :], fine_t[r : r + SUBS, :]
        shift = 1
        while shift < per_pixel:
            c = c + t * pltpu.roll(c, LANES - shift, 1)
            t = t * pltpu.roll(t, LANES - shift, 1)
            shift *= 2
        c, t = lanes_at(c, source), lanes_at(t, source)
        c, t = jnp.take_along_axis(c, group, axis=0)[0:1], jnp.take_along_axis(t, group, axis=0)[0:1]
        row = r // SUBS
        c0, t0 = coarse_c[row : row + 1, :], coarse_t[row : row + 1, :]
        to, at = row // level_rows, row % level_rows
        slab_ref[to, at : at + 1, :] = c0 + t0 * c
        slab_ref[to, level_rows + at : level_rows + at + 1, :] = t0 * t


def frame_kernel(n_morton, n_level, cap_f, cap_c, *refs):
    ints, tables, out_ref, refs = refs[:9], refs[9:13], refs[13], refs[14:]
    int_refs, table_refs, refs = refs[:9], refs[9:13], refs[13:]
    (
        owner_ref,
        fcode_ref,
        frank_ref,
        fcell_ref,
        flane_ref,
        group_ref,
        ccode_ref,
        crank_ref,
        ccell_ref,
        clane_ref,
        ones_ref,
        within_ref,
        ft_ref,
        ct_ref,
        left_ref,
        fc_ref,
        ftr_ref,
        cc_ref,
        ctr_ref,
        msg_ref,
        code_ref,
        served_ref,
        resp_ref,
        slab_ref,
        slabs_ref,
        ask_send,
        ask_recv,
        tell_send,
        tell_recv,
        join_send,
        join_recv,
        in_sems,
        *refs,
    ) = refs
    even, odd = refs
    n_dev = n_morton * n_level
    nf, nc = cap_f // LANES, cap_c // LANES
    blocks = nf + nc
    copies = [
        pltpu.make_async_copy(src, dst, in_sems.at[i])
        for i, (src, dst) in enumerate(zip(ints + tables, int_refs + table_refs))
    ]
    for copy in copies[:9]:
        copy.start()
    morton, level = lax.axis_index("morton"), lax.axis_index("level")
    me = morton * n_level + level
    mesh_ids = pl.DeviceIdType.MESH

    def device(d):
        return d // n_level, lax.rem(d, n_level)

    def wrap(x, n):
        return jnp.where(x >= n, x - n, x)

    def others(act):
        levels = [wrap(level + k, n_level) for k in range(n_level)]
        for there in levels[1:]:
            act(morton, there)

        def group(k, _):
            for there in levels:
                act(wrap(morton + k, n_morton), there)
            return 0

        lax.fori_loop(1, n_morton, group, 0)

    def ask(there, source):
        return pltpu.make_async_remote_copy(
            src_ref=msg_ref.at[there[0] * n_level + there[1]],
            dst_ref=code_ref.at[me],
            send_sem=ask_send.at[there[0] * n_level + there[1]],
            recv_sem=ask_recv.at[source],
            device_id=there,
            device_id_type=mesh_ids,
        )

    def tell(there, source):
        return pltpu.make_async_remote_copy(
            src_ref=served_ref.at[there[0] * n_level + there[1]],
            dst_ref=resp_ref.at[me],
            send_sem=tell_send.at[there[0] * n_level + there[1]],
            recv_sem=tell_recv.at[source],
            device_id=there,
            device_id_type=mesh_ids,
        )

    partner = level + 1 - 2 * lax.rem(level, 2)
    row, column_in = morton // 2, lax.rem(morton, 2)
    ordered = n_morton % 2 == 0 and n_morton >= 6 and n_level % 2 == 0

    def source(t):
        if not ordered:
            return lax.rem(me + n_dev - t, n_dev)
        n_rows = n_morton // 2
        g, turn = (t - 1) // n_level, lax.rem(t - 1, n_level)
        first = row == 0
        u = jnp.maximum(jnp.where(first, g - 1, g - 2), 0)
        far = 2 * (1 + lax.rem(row + u // 2, n_rows - 1)) + lax.rem(u + column_in, 2)
        head = jnp.where(first, g < 1, g < 2)
        group = jnp.where(head, jnp.where(first, 1 - column_in, g), far)
        group = jnp.where((row > 0) & (g == n_morton - 2), 2 * row + 1 - column_in, group)
        i = t - (n_dev - n_level + 1)
        near = jnp.where(lax.rem(i, 2) == 0, level, partner) + 2 * (i // 2 + 1)
        near = jnp.where(t == n_dev - 1, partner, lax.rem(near, n_level))
        away = group * n_level + wrap(level + turn, n_level)
        return jnp.where(t == 0, me, jnp.where(i >= 0, morton * n_level + near, away))

    def join(k):
        to = lax.rem(level + k, n_level)
        return pltpu.make_async_remote_copy(
            src_ref=slab_ref.at[to],
            dst_ref=slabs_ref.at[level],
            send_sem=join_send.at[k],
            recv_sem=join_recv.at[k],
            device_id=(morton, to),
            device_id_type=mesh_ids,
        )

    def after(k):
        return wrap(me + k, n_dev)

    barrier = pltpu.get_barrier_semaphore()

    def each(low, high, act):
        def body(k, _):
            act(k)
            return 0

        lax.fori_loop(low, high, body, 0)

    others(lambda m, l: pl.semaphore_signal(barrier, inc=1, device_id=(m, l), device_id_type=mesh_ids))
    for copy in copies[9:]:
        copy.start()
    for copy in copies[:9]:
        copy.wait()
    f_owner, f_brick, f_lane, f_entry, f_count, c_brick, c_lane, c_entry, c_count = int_refs

    owner_ref[...] = f_owner[...]
    fcode_ref[...] = (((f_brick[...] * COLUMNS + f_lane[...]) * BRICK + f_entry[...]) << 6) + f_count[...]
    rank_rows(owner_ref, n_dev, ones_ref, within_ref, frank_ref)
    rank = frank_ref[...]
    fcell_ref[...] = f_owner[...] * nf + rank // LANES
    flane_ref[...] = rank & (LANES - 1)
    fine_msg = place(fcell_ref, flane_ref, fcode_ref, n_dev * nf, SUBS)

    c_cols = table_refs[2].shape[0] * PER_ROW
    column = c_brick[...] * COLUMNS + c_lane[...]
    group_ref[...] = column // c_cols
    ccode_ref[...] = (((column & (c_cols - 1)) * BRICK + c_entry[...]) << 6) + c_count[...]
    rank_rows(group_ref, n_morton, ones_ref, within_ref, crank_ref)
    rank = crank_ref[...]
    slot = rank // n_level
    dest = group_ref[...] * n_level + (rank & (n_level - 1))
    ccell_ref[...] = dest * nc + slot // LANES
    clane_ref[...] = slot & (LANES - 1)
    coarse_msg = place(ccell_ref, clane_ref, ccode_ref, n_dev * nc, SUBS)
    for i in range(n_dev):
        msg_ref[i, :nf, :] = fine_msg[i * nf : (i + 1) * nf]
        msg_ref[i, nf:, :] = coarse_msg[i * nc : (i + 1) * nc]

    pl.semaphore_wait(barrier, n_dev - 1)
    others(lambda m, l: ask((m, l), me).start())
    code_ref[me] = msg_ref[me]
    for copy in copies[9:]:
        copy.wait()
    fd_ref, fe_ref, cd_ref, ce_ref = table_refs
    turn_tables(ft_ref, fd_ref, fe_ref, ct_ref, cd_ref, ce_ref)

    def codes_of(i, at, rows):
        return jnp.concatenate([code_ref[i, at + r : at + r + 1, :] for r in range(rows)], axis=1)

    def put(i, b, c, t):
        served_ref[i, b : b + 1, :] = c
        served_ref[i, blocks + b : blocks + b + 1, :] = t

    def fetch_source(i, buf):
        fetch(codes_of(i, 0, nf), ft_ref, buf)
        for b in range(nf, blocks):
            put(i, b, *march_lanes(code_ref[i, b : b + 1, :], ct_ref))

    def march_source(i, buf):
        for b in range(nf):
            put(i, b, *march(code_ref[i, b : b + 1, :], buf, b * LANES))

    odd[...] = jnp.zeros(odd.shape, F32)

    def await_ask(d):
        ask((morton, level), d).wait_recv()

    def start_tell(d):
        tell(device(d), me).start()

    def two_sources(j, state):
        older, old, last, now, later = state

        @pl.when(j > 0)
        def _():
            await_ask(now)

        @pl.when(j > 1)
        def _():
            start_tell(older)

        await_ask(later)

        @pl.when(j > 1)
        def _():
            start_tell(old)

        fetch_source(now, even)
        march_source(last, odd)
        fetch_source(later, odd)
        march_source(now, even)
        ahead = jnp.minimum(2 * j + 2, n_dev - 2)
        return last, now, later, source(ahead), source(ahead + 1)

    state = (me, me, me, me, source(1))
    older, old, last, _, _ = lax.fori_loop(0, n_dev // 2, two_sources, state)
    start_tell(older)
    start_tell(old)
    march_source(last, odd)
    start_tell(last)
    resp_ref[me] = served_ref[me]
    rank = frank_ref[...]
    wf, wc = min(nf, 2), min(nc, 2)
    fcell_ref[...] = owner_ref[...] + (rank // (wf * LANES)) * n_dev
    flane_ref[...] = rank & (wf * LANES - 1)
    rank = crank_ref[...]
    slot = rank // n_level
    ccell_ref[...] = group_ref[...] * n_level + (rank & (n_level - 1)) + (slot // (wc * LANES)) * n_dev
    clane_ref[...] = slot & (wc * LANES - 1)
    each(1, n_dev, lambda k: tell((morton, level), after(k)).wait_recv())
    look_up(resp_ref, nf, nc, wc, ccell_ref, clane_ref, left_ref, (cc_ref, ctr_ref))
    look_up(resp_ref, 0, nf, wf, fcell_ref, flane_ref, left_ref, (fc_ref, ftr_ref))
    blend(owner_ref.shape[0] // group_ref.shape[0], fc_ref, ftr_ref, cc_ref, ctr_ref, slab_ref)
    for k in range(1, n_level):
        join(k).start()
    slabs_ref[level] = slab_ref[level]
    each(1, n_dev, lambda k: ask(device(after(k)), me).wait_send())
    each(1, n_dev, lambda k: tell(device(after(k)), me).wait_send())
    for k in range(1, n_level):
        join(k).wait()
    rows = out_ref.shape[1]
    color, trans = slabs_ref[0, :rows, :], slabs_ref[0, rows:, :]
    for s in range(1, n_level):
        color = color + trans * slabs_ref[s, :rows, :]
        trans = trans * slabs_ref[s, rows:, :]
    out_ref[0] = color
    out_ref[1] = trans


def shards(
    coarse_density,
    coarse_emission,
    fine_density,
    fine_emission,
    coarse_brick,
    coarse_lane,
    coarse_entry,
    coarse_count,
    fine_owner,
    fine_brick,
    fine_lane,
    fine_entry,
    fine_count,
):
    n_morton = lax.axis_size("morton")
    n_level = lax.axis_size("level")
    n_dev = n_morton * n_level
    segments = fine_brick.shape[0]
    pixels = coarse_brick.shape[0]
    cap_f = -(-(2 * segments // n_dev) // LANES) * LANES
    cap_c = -(-pixels // (n_level * LANES)) * LANES
    nf, nc = cap_f // LANES, cap_c // LANES
    blocks = nf + nc
    f_rows, c_rows = segments // LANES, pixels // LANES
    level_rows = c_rows // n_level
    ints = [x.reshape(f_rows, LANES) for x in (fine_owner, fine_brick, fine_lane, fine_entry, fine_count)]
    ints += [x.reshape(c_rows, LANES) for x in (coarse_brick, coarse_lane, coarse_entry, coarse_count)]
    tables = [fine_density, fine_emission, coarse_density, coarse_emission]
    t_rows, g_rows = fine_density.shape[0], coarse_density.shape[0]
    wide = max(f_rows * n_dev, c_rows * n_morton)
    left_rows = 4 * n_dev * max(nf // min(nf, 2), nc // min(nc, 2))

    def like(x):
        return pltpu.VMEM(x.shape, x.dtype)

    sems = [pltpu.SemaphoreType.DMA((n_dev,))] * 4 + [pltpu.SemaphoreType.DMA((n_level,))] * 2
    image = pl.pallas_call(
        functools.partial(frame_kernel, n_morton, n_level, cap_f, cap_c),
        out_shape=jax.ShapeDtypeStruct((2, level_rows, LANES), F32),
        in_specs=[ANY] * 13,
        out_specs=VMEM,
        scratch_shapes=[like(x) for x in ints + tables]
        + [pltpu.VMEM((f_rows, LANES), I32)] * 5
        + [pltpu.VMEM((c_rows, LANES), I32)] * 5
        + [
            pltpu.VMEM((wide, LANES), BF16),
            pltpu.VMEM((wide, 2 * LANES), F32),
            pltpu.VMEM((4 * LANES, t_rows), BF16),
            pltpu.VMEM((-(-g_rows // LANES) * PER_ROW * 2 * BRICK, LANES), F32),
            pltpu.VMEM((left_rows, 2 * LANES), BF16),
        ]
        + [pltpu.VMEM((f_rows, LANES), F32)] * 2
        + [pltpu.VMEM((c_rows, LANES), F32)] * 2
        + [
            pltpu.VMEM((n_dev, blocks, LANES), I32),
            pltpu.VMEM((n_dev, blocks, LANES), I32),
            pltpu.VMEM((n_dev, 2 * blocks, LANES), F32),
            pltpu.VMEM((n_dev, 2 * blocks, LANES), F32),
            pltpu.VMEM((n_level, 2 * level_rows, LANES), F32),
            pltpu.VMEM((n_level, 2 * level_rows, LANES), F32),
        ]
        + sems
        + [pltpu.SemaphoreType.DMA((13,))]
        + [pltpu.VMEM((2 * LANES, cap_f), F32)] * 2,
        compiler_params=pltpu.CompilerParams(collective_id=0, has_side_effects=True),
    )(*ints, *tables)
    return image[0].reshape(-1), image[1].reshape(-1)


def solution(mesh):
    both = P(("morton", "level"))
    rows = P(("morton", "level"), None)
    coarse = P("morton", None)
    return jax.shard_map(
        shards,
        mesh=mesh,
        in_specs=(coarse, coarse, rows, rows, both, both, both, both, rows, both, both, both, both),
        out_specs=(both, both),
        check_vma=False,
    )
```

```python
import functools

import jax
import jax.numpy as jnp
from jax import lax
from jax.experimental import pallas as pl
from jax.experimental.pallas import tpu as pltpu
from jax.sharding import PartitionSpec as P

BRICK = 32
LANES = 128
SUBS = 8
PER_ROW = LANES // BRICK
COLUMNS = BRICK**2
F32 = jnp.float32
BF16 = jnp.bfloat16
I32 = jnp.int32
I16 = jnp.int16
VMEM = pl.BlockSpec(memory_space=pltpu.VMEM)
ANY = pl.BlockSpec(memory_space=pl.ANY)


def iota(shape, dim):
    return lax.broadcasted_iota(I32, shape, dim)


def equals(ids, width):
    return iota((width, ids.shape[1]), 0).astype(I16) == ids.astype(I16)


def onehot(ids, width):
    return jnp.where(equals(ids, width), jnp.ones((), BF16), jnp.zeros((), BF16))


def split(x, parts):
    out = []
    for _ in range(parts):
        piece = x.astype(BF16)
        out.append(piece)
        x = x - piece.astype(F32)
    return out


def dot_nt(a, b):
    return lax.dot_general(a, b, (((1,), (1,)), ((), ())), preferred_element_type=F32)


def dot_nn(a, b):
    return jnp.dot(a, b, preferred_element_type=F32)


def across(ref, at, rows):
    return jnp.concatenate([ref[at + r : at + r + 1, :] for r in range(rows)], axis=1)


def rank_rows(ids_ref, width, ones_ref, within_ref, out_ref):
    rows = ids_ref.shape[0]
    for r in range(rows):
        ones_ref[r * width : (r + 1) * width, :] = onehot(ids_ref[r : r + 1, :], width)
    lane, other = iota((LANES, 2 * LANES), 0), iota((LANES, 2 * LANES), 1)
    counter = jnp.where((lane < other) | (other >= LANES), 1.0, 0.0).astype(BF16)
    used = rows * width
    within_ref[:used, :] = dot_nn(ones_ref[:used, :], counter)
    ids_of = iota((width, LANES), 0)
    carry = jnp.zeros((width, LANES), F32)
    for r in range(rows):
        part = within_ref[r * width : (r + 1) * width, :]
        mine = jnp.where(ids_of == ids_ref[r : r + 1, :], part[:, :LANES] + carry, 0.0)
        out_ref[r : r + 1, :] = jnp.sum(mine, axis=0, keepdims=True).astype(I32)
        carry = carry + part[:, LANES:]


def to_float(value):
    return ((LANES + (value & (LANES - 1))) << (value >> 7)).astype(F32)


def from_float(x):
    y = x.astype(I32)
    shift = jnp.zeros_like(y)
    for bits in (8, 4, 2, 1):
        over = y >= (LANES << bits)
        y = jnp.where(over, y >> bits, y)
        shift = jnp.where(over, shift + bits, shift)
    return jnp.where(y == 0, 0, y - LANES + (shift << 7))


def place(cell_ref, lane_ref, code_ref, cells, chunk):
    rows = cell_ref.shape[0]
    placed = jnp.zeros((2 * cells, LANES), F32)
    for r in range(0, rows, chunk):
        here = equals(across(cell_ref, r, chunk), cells)
        code = across(code_ref, r, chunk)
        pieces = [to_float(code >> 11).astype(BF16), to_float(code & 2047).astype(BF16)]
        left = jnp.concatenate([jnp.where(here, p, jnp.zeros((), BF16)) for p in pieces], axis=0)
        right = onehot(across(lane_ref, r, chunk), LANES)
        placed = placed + dot_nt(left, right)
    return (from_float(placed[:cells]) << 11) + from_float(placed[cells:])


def cells_of(shape):
    rows = iota(shape, 0)
    return (rows & -BRICK) + 4 * (rows & 7) + ((rows >> 3) & 3)


def turned(turn, ref, parts):
    return [dot_nt(turn, piece) for piece in split(ref[...], parts)]


def turn_tables(ft_ref, fd_ref, fe_ref, ct_ref, cd_ref, ce_ref):
    turn = jnp.where(cells_of((LANES, LANES)) == iota((LANES, LANES), 1), 1.0, 0.0).astype(BF16)
    for at, ref in ((0, fd_ref), (LANES, fe_ref)):
        for i, piece in enumerate(turned(turn, ref, 2)):
            top = 2 * LANES * i + at
            ft_ref[top : top + LANES, :] = piece.astype(BF16)
    wide = ct_ref.shape[0] // PER_ROW
    rows = cd_ref.shape[0]
    for v, ref in enumerate((cd_ref, ce_ref)):
        whole = sum(turned(turn, ref, 3))
        for q in range(PER_ROW):
            for at in range(0, rows, LANES):
                size = min(LANES, rows - at)
                top = q * wide + (at // LANES) * 2 * BRICK + v * BRICK
                ct_ref[top : top + BRICK, :size] = whole[q * BRICK : (q + 1) * BRICK, at : at + size]


def fetch(codes, table_ref, got_ref):
    ones = onehot(codes >> 13, table_ref.shape[1])
    both = dot_nn(table_ref[...], ones)
    got_ref[...] = both[: 2 * LANES] + both[2 * LANES :]


def lanes_at(x, lanes):
    return jnp.take_along_axis(x, lanes, axis=1)


def front_to_back(dens, emis):
    trans = [jnp.exp(-d) for d in dens]
    color = [(1.0 - t) * e for t, e in zip(trans, emis)]
    c, t = color[3], trans[3]
    for k in (2, 1, 0):
        c = color[k] + trans[k] * c
        t = trans[k] * t
    for shift in (1, 2, 4):
        c = c + t * pltpu.roll(c, SUBS - shift, 0)
        t = t * pltpu.roll(t, SUBS - shift, 0)
    return c[0:1], t[0:1]


def march(codes, got_ref, at):
    first = (codes >> 6) & 127
    last = first + (codes & 63)
    cells = cells_of((LANES, LANES))
    inside = (cells >= first) & (cells < last)
    dens = jnp.where(inside, got_ref[:LANES, at : at + LANES], 0.0)
    emis = jnp.where(inside, got_ref[LANES:, at : at + LANES], 0.0)
    dens = sum(dens[g * BRICK : (g + 1) * BRICK] for g in range(PER_ROW))
    emis = sum(emis[g * BRICK : (g + 1) * BRICK] for g in range(PER_ROW))
    steps = range(0, BRICK, SUBS)
    return front_to_back([dens[k : k + SUBS] for k in steps], [emis[k : k + SUBS] for k in steps])


def march_lanes(codes, table_ref):
    codes = jnp.broadcast_to(codes, (SUBS, LANES))
    row = codes >> 13
    wide = table_ref.shape[0] // (PER_ROW * 2 * BRICK)
    group = ((codes >> 11) & (PER_ROW - 1)) * wide + row // LANES
    lane = row & (LANES - 1)
    got = [None] * (2 * BRICK // SUBS)
    for g in range(PER_ROW * wide):
        here = group == g
        for v in range(len(got)):
            top = g * 2 * BRICK + v * SUBS
            value = lanes_at(table_ref[top : top + SUBS, :], lane)
            got[v] = value if g == 0 else jnp.where(here, value, got[v])
    first = (codes >> 6) & (BRICK - 1)
    last = first + (codes & 63)
    steps = BRICK // SUBS
    cells = [steps * iota((SUBS, LANES), 0) + k for k in range(steps)]
    inside = [(c >= first) & (c < last) for c in cells]
    dens = [jnp.where(m, x, 0.0) for m, x in zip(inside, got[:steps])]
    return front_to_back(dens, got[steps:])


def look_up(resp_ref, near, at, blocks, width, owner_ref, rank_ref, left_ref, out_refs):
    half = resp_ref.shape[1] // 2
    owners = resp_ref.shape[0] - near
    high = blocks // width
    cells = high * owners
    for v in range(2):
        for h in range(high):
            for w in range(width):
                full = resp_ref[near:, v * half + at + h * width + w, :]
                for i, piece in enumerate(split(full, 2)):
                    top = (2 * v + i) * cells + h * owners
                    left_ref[top : top + owners, w * LANES : (w + 1) * LANES] = piece
    rows = owner_ref.shape[0]
    chunk = SUBS
    left = left_ref[: 4 * cells, : width * LANES]
    for r in range(0, rows, chunk):
        owner, rank = across(owner_ref, r, chunk), across(rank_ref, r, chunk)
        got = dot_nn(left, onehot(rank & (width * LANES - 1), width * LANES))
        cell = jnp.where(owner >= near, owner - near + rank // (width * LANES) * owners, -1)
        here = iota((cells, chunk * LANES), 0) == cell
        for v in range(2):
            total = got[2 * v * cells : (2 * v + 1) * cells] + got[(2 * v + 1) * cells : (2 * v + 2) * cells]
            value = jnp.sum(jnp.where(here, total, 0.0), axis=0, keepdims=True)
            for j in range(chunk):
                out_refs[v][r + j : r + j + 1, :] = value[:, j * LANES : (j + 1) * LANES]


def look_near(resp_ref, near, at, blocks, owner_ref, rank_ref, out_refs):
    half = resp_ref.shape[1] // 2
    for r in range(0, owner_ref.shape[0], SUBS):
        rank = rank_ref[r : r + SUBS, :]
        cell = owner_ref[r : r + SUBS, :] * blocks + rank // LANES
        lane = rank & (LANES - 1)
        values = [ref[r : r + SUBS, :] for ref in out_refs]
        for d in range(near):
            for b in range(blocks):
                here = cell == d * blocks + b
                for v in range(2):
                    row = resp_ref[d, v * half + at + b : v * half + at + b + 1, :]
                    value = lanes_at(jnp.broadcast_to(row, (SUBS, LANES)), lane)
                    values[v] = jnp.where(here, value, values[v])
        for ref, value in zip(out_refs, values):
            ref[r : r + SUBS, :] = value


def blend(per_pixel, fine_c, fine_t, coarse_c, coarse_t, slab_ref):
    rows = fine_c.shape[0]
    level_rows = slab_ref.shape[1] // 2
    pixel_lanes = LANES // per_pixel
    lane = iota((SUBS, LANES), 1)
    source = (lane & (pixel_lanes - 1)) * per_pixel
    group = lane // pixel_lanes
    for r in range(0, rows, SUBS):
        c, t = fine_c[r : r + SUBS, :], fine_t[r : r + SUBS, :]
        shift = 1
        while shift < per_pixel:
            c = c + t * pltpu.roll(c, LANES - shift, 1)
            t = t * pltpu.roll(t, LANES - shift, 1)
            shift *= 2
        c, t = lanes_at(c, source), lanes_at(t, source)
        c, t = jnp.take_along_axis(c, group, axis=0)[0:1], jnp.take_along_axis(t, group, axis=0)[0:1]
        row = r // SUBS
        c0, t0 = coarse_c[row : row + 1, :], coarse_t[row : row + 1, :]
        to, at = row // level_rows, row % level_rows
        slab_ref[to, at : at + 1, :] = c0 + t0 * c
        slab_ref[to, level_rows + at : level_rows + at + 1, :] = t0 * t


def frame_kernel(n_morton, n_level, cap_f, cap_c, *refs):
    ints, tables, out_ref, refs = refs[:9], refs[9:13], refs[13], refs[14:]
    int_refs, table_refs, refs = refs[:9], refs[9:13], refs[13:]
    (
        owner_ref,
        fcode_ref,
        frank_ref,
        fcell_ref,
        flane_ref,
        group_ref,
        ccode_ref,
        crank_ref,
        ccell_ref,
        clane_ref,
        ones_ref,
        within_ref,
        ft_ref,
        ct_ref,
        left_ref,
        fc_ref,
        ftr_ref,
        cc_ref,
        ctr_ref,
        msg_ref,
        code_ref,
        served_ref,
        resp_ref,
        slab_ref,
        slabs_ref,
        ask_send,
        ask_recv,
        tell_send,
        tell_recv,
        join_send,
        join_recv,
        in_sems,
        *refs,
    ) = refs
    even, odd = refs
    n_dev = n_morton * n_level
    nf, nc = cap_f // LANES, cap_c // LANES
    blocks = nf + nc
    copies = [
        pltpu.make_async_copy(src, dst, in_sems.at[i])
        for i, (src, dst) in enumerate(zip(ints + tables, int_refs + table_refs))
    ]
    for copy in copies[:9]:
        copy.start()
    morton, level = lax.axis_index("morton"), lax.axis_index("level")
    me = morton * n_level + level
    mesh_ids = pl.DeviceIdType.MESH

    def device(d):
        return d // n_level, lax.rem(d, n_level)

    def wrap(x, n):
        return jnp.where(x >= n, x - n, x)

    def others(act):
        levels = [wrap(level + k, n_level) for k in range(n_level)]
        for there in levels[1:]:
            act(morton, there)

        def group(k, _):
            for there in levels:
                act(wrap(morton + k, n_morton), there)
            return 0

        lax.fori_loop(1, n_morton, group, 0)

    def ask(there, source):
        return pltpu.make_async_remote_copy(
            src_ref=msg_ref.at[there[0] * n_level + there[1]],
            dst_ref=code_ref.at[me],
            send_sem=ask_send.at[there[0] * n_level + there[1]],
            recv_sem=ask_recv.at[source],
            device_id=there,
            device_id_type=mesh_ids,
        )

    def tell(there, source):
        return pltpu.make_async_remote_copy(
            src_ref=served_ref.at[there[0] * n_level + there[1]],
            dst_ref=resp_ref.at[source],
            send_sem=tell_send.at[there[0] * n_level + there[1]],
            recv_sem=tell_recv.at[source],
            device_id=there,
            device_id_type=mesh_ids,
        )

    ordered = n_morton % 2 == 0 and n_morton >= 6 and n_level % 2 == 0
    near = 2 * n_level if ordered else 0
    partner = level + 1 - 2 * lax.rem(level, 2)
    row, column_in = morton // 2, lax.rem(morton, 2)

    def seen_by(d, m):
        return wrap(d + n_dev - m // 2 * near, n_dev)

    def source(t):
        if not ordered:
            return lax.rem(me + n_dev - t, n_dev)
        n_rows = n_morton // 2
        step = jnp.maximum(t - 2, 0)
        g, turn = step // n_level, lax.rem(step, n_level)
        first = row == 0
        u = jnp.maximum(jnp.where(first, g - 1, g - 2), 0)
        far = 2 * (1 + lax.rem(row + u // 2, n_rows - 1)) + lax.rem(u + column_in, 2)
        head = jnp.where(first, g < 1, g < 2)
        group = jnp.where(head, jnp.where(first, 1 - column_in, g), far)
        group = jnp.where((row > 0) & (g == n_morton - 2), 2 * row + 1 - column_in, group)
        i = t - (n_dev - n_level + 2)
        beside = lax.rem(jnp.where(lax.rem(i, 2) == 0, level, partner) + 2 * (i // 2 + 1), n_level)
        away = group * n_level + wrap(level + turn, n_level)
        far_or_beside = jnp.where(i >= 0, morton * n_level + beside, away)
        return jnp.where(t == 0, me, jnp.where(t == 1, morton * n_level + partner, far_or_beside))

    def join(k):
        to = lax.rem(level + k, n_level)
        return pltpu.make_async_remote_copy(
            src_ref=slab_ref.at[to],
            dst_ref=slabs_ref.at[level],
            send_sem=join_send.at[k],
            recv_sem=join_recv.at[k],
            device_id=(morton, to),
            device_id_type=mesh_ids,
        )

    def after(k):
        return wrap(me + k, n_dev)

    barrier = pltpu.get_barrier_semaphore()

    def each(low, high, act):
        def body(k, _):
            act(k)
            return 0

        lax.fori_loop(low, high, body, 0)

    others(lambda m, l: pl.semaphore_signal(barrier, inc=1, device_id=(m, l), device_id_type=mesh_ids))
    for copy in copies[9:]:
        copy.start()
    for copy in copies[:9]:
        copy.wait()
    f_owner, f_brick, f_lane, f_entry, f_count, c_brick, c_lane, c_entry, c_count = int_refs

    owner_ref[...] = f_owner[...]
    fcode_ref[...] = (((f_brick[...] * COLUMNS + f_lane[...]) * BRICK + f_entry[...]) << 6) + f_count[...]
    rank_rows(owner_ref, n_dev, ones_ref, within_ref, frank_ref)
    rank = frank_ref[...]
    fcell_ref[...] = f_owner[...] * nf + rank // LANES
    flane_ref[...] = rank & (LANES - 1)
    fine_msg = place(fcell_ref, flane_ref, fcode_ref, n_dev * nf, SUBS)

    c_cols = table_refs[2].shape[0] * PER_ROW
    column = c_brick[...] * COLUMNS + c_lane[...]
    group_ref[...] = column // c_cols
    ccode_ref[...] = (((column & (c_cols - 1)) * BRICK + c_entry[...]) << 6) + c_count[...]
    rank_rows(group_ref, n_morton, ones_ref, within_ref, crank_ref)
    rank = crank_ref[...]
    slot = rank // n_level
    dest = group_ref[...] * n_level + (rank & (n_level - 1))
    ccell_ref[...] = dest * nc + slot // LANES
    clane_ref[...] = slot & (LANES - 1)
    coarse_msg = place(ccell_ref, clane_ref, ccode_ref, n_dev * nc, SUBS)
    for i in range(n_dev):
        msg_ref[i, :nf, :] = fine_msg[i * nf : (i + 1) * nf]
        msg_ref[i, nf:, :] = coarse_msg[i * nc : (i + 1) * nc]

    pl.semaphore_wait(barrier, n_dev - 1)
    others(lambda m, l: ask((m, l), me).start())
    code_ref[me] = msg_ref[me]
    for copy in copies[9:]:
        copy.wait()
    fd_ref, fe_ref, cd_ref, ce_ref = table_refs
    turn_tables(ft_ref, fd_ref, fe_ref, ct_ref, cd_ref, ce_ref)

    def codes_of(i, at, rows):
        return jnp.concatenate([code_ref[i, at + r : at + r + 1, :] for r in range(rows)], axis=1)

    def put(i, b, c, t):
        served_ref[i, b : b + 1, :] = c
        served_ref[i, blocks + b : blocks + b + 1, :] = t

    def fetch_source(i, buf):
        fetch(codes_of(i, 0, nf), ft_ref, buf)
        for b in range(nf, blocks):
            put(i, b, *march_lanes(code_ref[i, b : b + 1, :], ct_ref))

    def march_source(i, buf):
        for b in range(nf):
            put(i, b, *march(code_ref[i, b : b + 1, :], buf, b * LANES))

    odd[...] = jnp.zeros(odd.shape, F32)

    def await_ask(d):
        ask((morton, level), d).wait_recv()

    def start_tell(d):
        there = device(d)
        tell(there, seen_by(me, there[0])).start()

    def two_sources(j, state):
        older, old, last, now, later = state

        @pl.when(j > 0)
        def _():
            await_ask(now)

        @pl.when(j > 1)
        def _():
            start_tell(older)

        await_ask(later)

        @pl.when(j > 1)
        def _():
            start_tell(old)

        fetch_source(now, even)
        march_source(last, odd)
        fetch_source(later, odd)
        march_source(now, even)
        ahead = jnp.minimum(2 * j + 2, n_dev - 2)
        return last, now, later, source(ahead), source(ahead + 1)

    state = (me, me, me, me, source(1))
    older, old, last, _, _ = lax.fori_loop(0, n_dev // 2, two_sources, state)
    start_tell(older)
    start_tell(old)
    march_source(last, odd)
    start_tell(last)
    mine = seen_by(me, morton)
    resp_ref[mine] = served_ref[me]
    seen = owner_ref[...] - row * near
    owner_ref[...] = jnp.where(seen < 0, seen + n_dev, seen)
    rank = crank_ref[...]
    seen = group_ref[...] * n_level + (rank & (n_level - 1)) - row * near
    ccell_ref[...] = jnp.where(seen < 0, seen + n_dev, seen)
    crank_ref[...] = rank // n_level

    def await_tells(low, high):
        def one(v, _):
            @pl.when(v != mine)
            def _():
                tell((morton, level), v).wait_recv()

            return 0

        lax.fori_loop(low, high, one, 0)

    await_tells(near, n_dev)
    fine, coarse = (owner_ref, frank_ref), (ccell_ref, crank_ref)
    look_up(resp_ref, near, nf, nc, min(nc, 2), *coarse, left_ref, (cc_ref, ctr_ref))
    look_up(resp_ref, near, 0, nf, min(nf, 2), *fine, left_ref, (fc_ref, ftr_ref))
    await_tells(0, near)
    look_near(resp_ref, near, nf, nc, *coarse, (cc_ref, ctr_ref))
    look_near(resp_ref, near, 0, nf, *fine, (fc_ref, ftr_ref))
    blend(owner_ref.shape[0] // group_ref.shape[0], fc_ref, ftr_ref, cc_ref, ctr_ref, slab_ref)
    for k in range(1, n_level):
        join(k).start()
    slabs_ref[level] = slab_ref[level]
    each(1, n_dev, lambda k: ask(device(after(k)), me).wait_send())
    each(1, n_dev, lambda k: tell(device(after(k)), me).wait_send())
    for k in range(1, n_level):
        join(k).wait()
    rows = out_ref.shape[1]
    color, trans = slabs_ref[0, :rows, :], slabs_ref[0, rows:, :]
    for s in range(1, n_level):
        color = color + trans * slabs_ref[s, :rows, :]
        trans = trans * slabs_ref[s, rows:, :]
    out_ref[0] = color
    out_ref[1] = trans


def shards(
    coarse_density,
    coarse_emission,
    fine_density,
    fine_emission,
    coarse_brick,
    coarse_lane,
    coarse_entry,
    coarse_count,
    fine_owner,
    fine_brick,
    fine_lane,
    fine_entry,
    fine_count,
):
    n_morton = lax.axis_size("morton")
    n_level = lax.axis_size("level")
    n_dev = n_morton * n_level
    segments = fine_brick.shape[0]
    pixels = coarse_brick.shape[0]
    cap_f = -(-(2 * segments // n_dev) // LANES) * LANES
    cap_c = -(-pixels // (n_level * LANES)) * LANES
    nf, nc = cap_f // LANES, cap_c // LANES
    blocks = nf + nc
    f_rows, c_rows = segments // LANES, pixels // LANES
    level_rows = c_rows // n_level
    ints = [x.reshape(f_rows, LANES) for x in (fine_owner, fine_brick, fine_lane, fine_entry, fine_count)]
    ints += [x.reshape(c_rows, LANES) for x in (coarse_brick, coarse_lane, coarse_entry, coarse_count)]
    tables = [fine_density, fine_emission, coarse_density, coarse_emission]
    t_rows, g_rows = fine_density.shape[0], coarse_density.shape[0]
    wide = max(f_rows * n_dev, c_rows * n_morton)
    left_rows = 4 * n_dev * max(nf // min(nf, 2), nc // min(nc, 2))

    def like(x):
        return pltpu.VMEM(x.shape, x.dtype)

    sems = [pltpu.SemaphoreType.DMA((n_dev,))] * 4 + [pltpu.SemaphoreType.DMA((n_level,))] * 2
    image = pl.pallas_call(
        functools.partial(frame_kernel, n_morton, n_level, cap_f, cap_c),
        out_shape=jax.ShapeDtypeStruct((2, level_rows, LANES), F32),
        in_specs=[ANY] * 13,
        out_specs=VMEM,
        scratch_shapes=[like(x) for x in ints + tables]
        + [pltpu.VMEM((f_rows, LANES), I32)] * 5
        + [pltpu.VMEM((c_rows, LANES), I32)] * 5
        + [
            pltpu.VMEM((wide, LANES), BF16),
            pltpu.VMEM((wide, 2 * LANES), F32),
            pltpu.VMEM((4 * LANES, t_rows), BF16),
            pltpu.VMEM((-(-g_rows // LANES) * PER_ROW * 2 * BRICK, LANES), F32),
            pltpu.VMEM((left_rows, 2 * LANES), BF16),
        ]
        + [pltpu.VMEM((f_rows, LANES), F32)] * 2
        + [pltpu.VMEM((c_rows, LANES), F32)] * 2
        + [
            pltpu.VMEM((n_dev, blocks, LANES), I32),
            pltpu.VMEM((n_dev, blocks, LANES), I32),
            pltpu.VMEM((n_dev, 2 * blocks, LANES), F32),
            pltpu.VMEM((n_dev, 2 * blocks, LANES), F32),
            pltpu.VMEM((n_level, 2 * level_rows, LANES), F32),
            pltpu.VMEM((n_level, 2 * level_rows, LANES), F32),
        ]
        + sems
        + [pltpu.SemaphoreType.DMA((13,))]
        + [pltpu.VMEM((2 * LANES, cap_f), F32)] * 2,
        compiler_params=pltpu.CompilerParams(collective_id=0, has_side_effects=True),
    )(*ints, *tables)
    return image[0].reshape(-1), image[1].reshape(-1)


def solution(mesh):
    both = P(("morton", "level"))
    rows = P(("morton", "level"), None)
    coarse = P("morton", None)
    return jax.shard_map(
        shards,
        mesh=mesh,
        in_specs=(coarse, coarse, rows, rows, both, both, both, both, rows, both, both, both, both),
        out_specs=(both, both),
        check_vma=False,
    )
```

```python
import functools

import jax
import jax.numpy as jnp
from jax import lax
from jax.experimental import pallas as pl
from jax.experimental.pallas import tpu as pltpu
from jax.sharding import PartitionSpec as P

BRICK = 32
LANES = 128
SUBS = 8
PER_ROW = LANES // BRICK
COLUMNS = BRICK**2
F32 = jnp.float32
BF16 = jnp.bfloat16
I32 = jnp.int32
I16 = jnp.int16
VMEM = pl.BlockSpec(memory_space=pltpu.VMEM)
ANY = pl.BlockSpec(memory_space=pl.ANY)


def iota(shape, dim):
    return lax.broadcasted_iota(I32, shape, dim)


def equals(ids, width):
    return iota((width, ids.shape[1]), 0).astype(I16) == ids.astype(I16)


def onehot(ids, width):
    return jnp.where(equals(ids, width), jnp.ones((), BF16), jnp.zeros((), BF16))


def split(x, parts):
    out = []
    for _ in range(parts):
        piece = x.astype(BF16)
        out.append(piece)
        x = x - piece.astype(F32)
    return out


def dot_nt(a, b):
    return lax.dot_general(a, b, (((1,), (1,)), ((), ())), preferred_element_type=F32)


def dot_nn(a, b):
    return jnp.dot(a, b, preferred_element_type=F32)


def across(ref, at, rows):
    return jnp.concatenate([ref[at + r : at + r + 1, :] for r in range(rows)], axis=1)


def rank_rows(ids_ref, width, ones_ref, within_ref, out_ref):
    rows = ids_ref.shape[0]
    for r in range(rows):
        ones_ref[r * width : (r + 1) * width, :] = onehot(ids_ref[r : r + 1, :], width)
    lane, other = iota((LANES, 2 * LANES), 0), iota((LANES, 2 * LANES), 1)
    counter = jnp.where((lane < other) | (other >= LANES), 1.0, 0.0).astype(BF16)
    used = rows * width
    within_ref[:used, :] = dot_nn(ones_ref[:used, :], counter)
    ids_of = iota((width, LANES), 0)
    carry = jnp.zeros((width, LANES), F32)
    for r in range(rows):
        part = within_ref[r * width : (r + 1) * width, :]
        mine = jnp.where(ids_of == ids_ref[r : r + 1, :], part[:, :LANES] + carry, 0.0)
        out_ref[r : r + 1, :] = jnp.sum(mine, axis=0, keepdims=True).astype(I32)
        carry = carry + part[:, LANES:]


def to_float(value):
    return ((LANES + (value & (LANES - 1))) << (value >> 7)).astype(F32)


def from_float(x):
    y = x.astype(I32)
    shift = jnp.zeros_like(y)
    for bits in (8, 4, 2, 1):
        over = y >= (LANES << bits)
        y = jnp.where(over, y >> bits, y)
        shift = jnp.where(over, shift + bits, shift)
    return jnp.where(y == 0, 0, y - LANES + (shift << 7))


def place(cell_ref, lane_ref, code_ref, cells, chunk):
    rows = cell_ref.shape[0]
    placed = jnp.zeros((2 * cells, LANES), F32)
    for r in range(0, rows, chunk):
        here = equals(across(cell_ref, r, chunk), cells)
        code = across(code_ref, r, chunk)
        pieces = [to_float(code >> 11).astype(BF16), to_float(code & 2047).astype(BF16)]
        left = jnp.concatenate([jnp.where(here, p, jnp.zeros((), BF16)) for p in pieces], axis=0)
        right = onehot(across(lane_ref, r, chunk), LANES)
        placed = placed + dot_nt(left, right)
    return (from_float(placed[:cells]) << 11) + from_float(placed[cells:])


def cells_of(shape):
    rows = iota(shape, 0)
    return (rows & -BRICK) + 4 * (rows & 7) + ((rows >> 3) & 3)


def turned(turn, ref, parts):
    return [dot_nt(turn, piece) for piece in split(ref[...], parts)]


def turn_tables(ft_ref, fd_ref, fe_ref, ct_ref, cd_ref, ce_ref):
    turn = jnp.where(cells_of((LANES, LANES)) == iota((LANES, LANES), 1), 1.0, 0.0).astype(BF16)
    for at, ref in ((0, fd_ref), (LANES, fe_ref)):
        for i, piece in enumerate(turned(turn, ref, 2)):
            top = 2 * LANES * i + at
            ft_ref[top : top + LANES, :] = piece.astype(BF16)
    wide = ct_ref.shape[0] // PER_ROW
    rows = cd_ref.shape[0]
    for v, ref in enumerate((cd_ref, ce_ref)):
        whole = sum(turned(turn, ref, 3))
        for q in range(PER_ROW):
            for at in range(0, rows, LANES):
                size = min(LANES, rows - at)
                top = q * wide + (at // LANES) * 2 * BRICK + v * BRICK
                ct_ref[top : top + BRICK, :size] = whole[q * BRICK : (q + 1) * BRICK, at : at + size]


def fetch(codes, table_ref, got_ref):
    ones = onehot(codes >> 13, table_ref.shape[1])
    both = dot_nn(table_ref[...], ones)
    got_ref[...] = both[: 2 * LANES] + both[2 * LANES :]


def lanes_at(x, lanes):
    return jnp.take_along_axis(x, lanes, axis=1)


def front_to_back(dens, emis):
    trans = [jnp.exp(-d) for d in dens]
    color = [(1.0 - t) * e for t, e in zip(trans, emis)]
    c, t = color[3], trans[3]
    for k in (2, 1, 0):
        c = color[k] + trans[k] * c
        t = trans[k] * t
    for shift in (1, 2, 4):
        c = c + t * pltpu.roll(c, SUBS - shift, 0)
        t = t * pltpu.roll(t, SUBS - shift, 0)
    return c[0:1], t[0:1]


def march(codes, got_ref, at):
    codes = jnp.broadcast_to(codes, (SUBS, LANES))
    quarter = (codes >> 11) & (PER_ROW - 1)
    here = [quarter == q for q in range(PER_ROW - 1)]
    steps = BRICK // SUBS

    def column(top):
        out = []
        for k in range(steps):
            rows = [got_ref[top + q * BRICK + k * SUBS : top + q * BRICK + (k + 1) * SUBS, at : at + LANES] for q in range(PER_ROW)]
            x = rows[-1]
            for q in range(PER_ROW - 1):
                x = jnp.where(here[q], rows[q], x)
            out.append(x)
        return out

    return front_to_back(sampled(codes, column(0)), column(LANES))


def sampled(codes, dens):
    first = (codes >> 6) & (BRICK - 1)
    last = first + (codes & 63)
    steps = BRICK // SUBS
    cells = [steps * iota((SUBS, LANES), 0) + k for k in range(steps)]
    return [jnp.where((c >= first) & (c < last), x, 0.0) for c, x in zip(cells, dens)]


def march_lanes(codes, table_ref):
    codes = jnp.broadcast_to(codes, (SUBS, LANES))
    row = codes >> 13
    wide = table_ref.shape[0] // (PER_ROW * 2 * BRICK)
    group = ((codes >> 11) & (PER_ROW - 1)) * wide + row // LANES
    lane = row & (LANES - 1)
    got = [None] * (2 * BRICK // SUBS)
    for g in range(PER_ROW * wide):
        here = group == g
        for v in range(len(got)):
            top = g * 2 * BRICK + v * SUBS
            value = lanes_at(table_ref[top : top + SUBS, :], lane)
            got[v] = value if g == 0 else jnp.where(here, value, got[v])
    steps = BRICK // SUBS
    return front_to_back(sampled(codes, got[:steps]), got[steps:])


def look_up(resp_ref, near, at, blocks, width, owner_ref, rank_ref, left_ref, out_refs):
    half = resp_ref.shape[1] // 2
    owners = resp_ref.shape[0] - near
    high = blocks // width
    cells = high * owners
    for v in range(2):
        for h in range(high):
            for w in range(width):
                full = resp_ref[near:, v * half + at + h * width + w, :]
                for i, piece in enumerate(split(full, 2)):
                    top = (2 * v + i) * cells + h * owners
                    left_ref[top : top + owners, w * LANES : (w + 1) * LANES] = piece
    rows = owner_ref.shape[0]
    chunk = SUBS
    left = left_ref[: 4 * cells, : width * LANES]
    for r in range(0, rows, chunk):
        owner, rank = across(owner_ref, r, chunk), across(rank_ref, r, chunk)
        got = dot_nn(left, onehot(rank & (width * LANES - 1), width * LANES))
        cell = jnp.where(owner >= near, owner - near + rank // (width * LANES) * owners, -1)
        here = iota((cells, chunk * LANES), 0) == cell
        for v in range(2):
            total = got[2 * v * cells : (2 * v + 1) * cells] + got[(2 * v + 1) * cells : (2 * v + 2) * cells]
            value = jnp.sum(jnp.where(here, total, 0.0), axis=0, keepdims=True)
            for j in range(chunk):
                out_refs[v][r + j : r + j + 1, :] = value[:, j * LANES : (j + 1) * LANES]


def look_near(resp_ref, near, at, blocks, owner_ref, rank_ref, out_refs):
    half = resp_ref.shape[1] // 2
    for r in range(0, owner_ref.shape[0], SUBS):
        rank = rank_ref[r : r + SUBS, :]
        cell = owner_ref[r : r + SUBS, :] * blocks + rank // LANES
        lane = rank & (LANES - 1)
        values = [ref[r : r + SUBS, :] for ref in out_refs]
        for d in range(near):
            for b in range(blocks):
                here = cell == d * blocks + b
                for v in range(2):
                    row = resp_ref[d, v * half + at + b : v * half + at + b + 1, :]
                    value = lanes_at(jnp.broadcast_to(row, (SUBS, LANES)), lane)
                    values[v] = jnp.where(here, value, values[v])
        for ref, value in zip(out_refs, values):
            ref[r : r + SUBS, :] = value


def blend(per_pixel, fine_c, fine_t, coarse_c, coarse_t, slab_ref):
    rows = fine_c.shape[0]
    level_rows = slab_ref.shape[1] // 2
    pixel_lanes = LANES // per_pixel
    lane = iota((SUBS, LANES), 1)
    source = (lane & (pixel_lanes - 1)) * per_pixel
    group = lane // pixel_lanes
    for r in range(0, rows, SUBS):
        c, t = fine_c[r : r + SUBS, :], fine_t[r : r + SUBS, :]
        shift = 1
        while shift < per_pixel:
            c = c + t * pltpu.roll(c, LANES - shift, 1)
            t = t * pltpu.roll(t, LANES - shift, 1)
            shift *= 2
        c, t = lanes_at(c, source), lanes_at(t, source)
        c, t = jnp.take_along_axis(c, group, axis=0)[0:1], jnp.take_along_axis(t, group, axis=0)[0:1]
        row = r // SUBS
        c0, t0 = coarse_c[row : row + 1, :], coarse_t[row : row + 1, :]
        to, at = row // level_rows, row % level_rows
        slab_ref[to, at : at + 1, :] = c0 + t0 * c
        slab_ref[to, level_rows + at : level_rows + at + 1, :] = t0 * t


def frame_kernel(n_morton, n_level, cap_f, cap_c, *refs):
    ints, tables, out_ref, refs = refs[:9], refs[9:13], refs[13], refs[14:]
    int_refs, table_refs, refs = refs[:9], refs[9:13], refs[13:]
    (
        owner_ref,
        fcode_ref,
        frank_ref,
        fcell_ref,
        flane_ref,
        group_ref,
        ccode_ref,
        crank_ref,
        ccell_ref,
        clane_ref,
        ones_ref,
        within_ref,
        ft_ref,
        ct_ref,
        left_ref,
        fc_ref,
        ftr_ref,
        cc_ref,
        ctr_ref,
        msg_ref,
        code_ref,
        served_ref,
        resp_ref,
        slab_ref,
        slabs_ref,
        ask_send,
        ask_recv,
        tell_send,
        tell_recv,
        join_send,
        join_recv,
        in_sems,
        *refs,
    ) = refs
    even, odd = refs
    n_dev = n_morton * n_level
    nf, nc = cap_f // LANES, cap_c // LANES
    blocks = nf + nc
    copies = [
        pltpu.make_async_copy(src, dst, in_sems.at[i])
        for i, (src, dst) in enumerate(zip(ints + tables, int_refs + table_refs))
    ]
    for copy in copies[:9]:
        copy.start()
    morton, level = lax.axis_index("morton"), lax.axis_index("level")
    me = morton * n_level + level
    mesh_ids = pl.DeviceIdType.MESH

    def device(d):
        return d // n_level, lax.rem(d, n_level)

    def wrap(x, n):
        return jnp.where(x >= n, x - n, x)

    def others(act):
        levels = [wrap(level + k, n_level) for k in range(n_level)]
        for there in levels[1:]:
            act(morton, there)

        def group(k, _):
            for there in levels:
                act(wrap(morton + k, n_morton), there)
            return 0

        lax.fori_loop(1, n_morton, group, 0)

    def ask(there, source):
        return pltpu.make_async_remote_copy(
            src_ref=msg_ref.at[there[0] * n_level + there[1]],
            dst_ref=code_ref.at[me],
            send_sem=ask_send.at[there[0] * n_level + there[1]],
            recv_sem=ask_recv.at[source],
            device_id=there,
            device_id_type=mesh_ids,
        )

    def tell(there, source):
        return pltpu.make_async_remote_copy(
            src_ref=served_ref.at[there[0] * n_level + there[1]],
            dst_ref=resp_ref.at[source],
            send_sem=tell_send.at[there[0] * n_level + there[1]],
            recv_sem=tell_recv.at[source],
            device_id=there,
            device_id_type=mesh_ids,
        )

    ordered = n_morton % 2 == 0 and n_morton >= 6 and n_level % 2 == 0
    near = 2 * n_level if ordered else 0
    partner = level + 1 - 2 * lax.rem(level, 2)
    row, column_in = morton // 2, lax.rem(morton, 2)

    def seen_by(d, m):
        return wrap(d + n_dev - m // 2 * near, n_dev)

    def source(t):
        if not ordered:
            return lax.rem(me + n_dev - t, n_dev)
        n_rows = n_morton // 2
        step = jnp.maximum(t - 2, 0)
        g, turn = step // n_level, lax.rem(step, n_level)
        first = row == 0
        u = jnp.maximum(jnp.where(first, g - 1, g - 2), 0)
        down = jnp.maximum(n_rows - 2 - u // 2, 0)
        far = 2 * (1 + jnp.where(row == 1, down, lax.rem(row + u // 2, n_rows - 1))) + lax.rem(u + 1 + column_in, 2)
        head = jnp.where(first, g < 1, g < 2)
        group = jnp.where(head, jnp.where(first, 1 - column_in, g), far)
        group = jnp.where((row > 0) & (g == n_morton - 2), 2 * row + 1 - column_in, group)
        i = t - (n_dev - n_level + 2)
        beside = lax.rem(jnp.where(lax.rem(i, 2) == 0, level, partner) + 2 * (i // 2 + 1), n_level)
        same = jnp.where(lax.rem(turn, 2) == 0, level, partner)
        away = group * n_level + lax.rem(same + n_level - 2 * (turn // 2 + 1), n_level)
        far_or_beside = jnp.where(i >= 0, morton * n_level + beside, away)
        return jnp.where(t == 0, me, jnp.where(t == 1, morton * n_level + partner, far_or_beside))

    def join(k):
        to = lax.rem(level + k, n_level)
        return pltpu.make_async_remote_copy(
            src_ref=slab_ref.at[to],
            dst_ref=slabs_ref.at[level],
            send_sem=join_send.at[k],
            recv_sem=join_recv.at[k],
            device_id=(morton, to),
            device_id_type=mesh_ids,
        )

    def after(k):
        return wrap(me + k, n_dev)

    barrier = pltpu.get_barrier_semaphore()

    def each(low, high, act):
        def body(k, _):
            act(k)
            return 0

        lax.fori_loop(low, high, body, 0)

    def greet(m, _):
        for k in range(n_level):
            there = wrap(level + k, n_level)

            def one():
                pl.semaphore_signal(barrier, inc=1, device_id=(m, there), device_id_type=mesh_ids)

            one() if k else pl.when(m != morton)(one)
        return 0

    lax.fori_loop(0, n_morton, greet, 0)
    for copy in copies[9:]:
        copy.start()
    for copy in copies[:9]:
        copy.wait()
    f_owner, f_brick, f_lane, f_entry, f_count, c_brick, c_lane, c_entry, c_count = int_refs

    owner_ref[...] = f_owner[...]
    fcode_ref[...] = (((f_brick[...] * COLUMNS + f_lane[...]) * BRICK + f_entry[...]) << 6) + f_count[...]
    rank_rows(owner_ref, n_dev, ones_ref, within_ref, frank_ref)
    rank = frank_ref[...]
    fcell_ref[...] = f_owner[...] * nf + rank // LANES
    flane_ref[...] = rank & (LANES - 1)
    fine_msg = place(fcell_ref, flane_ref, fcode_ref, n_dev * nf, SUBS)

    c_cols = table_refs[2].shape[0] * PER_ROW
    column = c_brick[...] * COLUMNS + c_lane[...]
    group_ref[...] = column // c_cols
    ccode_ref[...] = (((column & (c_cols - 1)) * BRICK + c_entry[...]) << 6) + c_count[...]
    rank_rows(group_ref, n_morton, ones_ref, within_ref, crank_ref)
    rank = crank_ref[...]
    slot = rank // n_level
    dest = group_ref[...] * n_level + (rank & (n_level - 1))
    ccell_ref[...] = dest * nc + slot // LANES
    clane_ref[...] = slot & (LANES - 1)
    coarse_msg = place(ccell_ref, clane_ref, ccode_ref, n_dev * nc, SUBS)
    for i in range(n_dev):
        msg_ref[i, :nf, :] = fine_msg[i * nf : (i + 1) * nf]
        msg_ref[i, nf:, :] = coarse_msg[i * nc : (i + 1) * nc]

    pl.semaphore_wait(barrier, n_dev - 1)
    others(lambda m, l: ask((m, l), me).start())
    pltpu.make_async_copy(msg_ref.at[me], code_ref.at[me], ask_recv.at[me]).start()
    for copy in copies[9:]:
        copy.wait()
    fd_ref, fe_ref, cd_ref, ce_ref = table_refs
    turn_tables(ft_ref, fd_ref, fe_ref, ct_ref, cd_ref, ce_ref)

    def codes_of(i, at, rows):
        return jnp.concatenate([code_ref[i, at + r : at + r + 1, :] for r in range(rows)], axis=1)

    def put(i, b, c, t):
        served_ref[i, b : b + 1, :] = c
        served_ref[i, blocks + b : blocks + b + 1, :] = t

    def fetch_source(i, buf):
        fetch(codes_of(i, 0, nf), ft_ref, buf)
        for b in range(nf, blocks):
            put(i, b, *march_lanes(code_ref[i, b : b + 1, :], ct_ref))

    def march_source(i, buf):
        for b in range(nf):
            put(i, b, *march(code_ref[i, b : b + 1, :], buf, b * LANES))

    odd[...] = jnp.zeros(odd.shape, F32)

    def await_ask(d):
        ask((morton, level), d).wait_recv()

    def start_tell(d):
        there = device(d)
        tell(there, seen_by(me, there[0])).start()

    def two_sources(j, state):
        older, old, last, now, later = state

        @pl.when(j > 1)
        def _():
            start_tell(older)
            start_tell(old)

        await_ask(now)
        await_ask(later)
        fetch_source(now, even)
        march_source(last, odd)
        fetch_source(later, odd)
        march_source(now, even)
        ahead = jnp.minimum(2 * j + 2, n_dev - 2)
        return last, now, later, source(ahead), source(ahead + 1)

    state = (me, me, me, me, source(1))
    older, old, last, _, _ = lax.fori_loop(0, n_dev // 2, two_sources, state)
    start_tell(older)
    start_tell(old)
    march_source(last, odd)
    start_tell(last)
    mine = seen_by(me, morton)
    resp_ref[mine] = served_ref[me]
    seen = owner_ref[...] - row * near
    owner_ref[...] = jnp.where(seen < 0, seen + n_dev, seen)
    rank = crank_ref[...]
    seen = group_ref[...] * n_level + (rank & (n_level - 1)) - row * near
    ccell_ref[...] = jnp.where(seen < 0, seen + n_dev, seen)
    crank_ref[...] = rank // n_level

    def await_tells(low, high):
        def one(v, _):
            @pl.when(v != mine)
            def _():
                tell((morton, level), v).wait_recv()

            return 0

        lax.fori_loop(low, high, one, 0)

    await_tells(near, n_dev)
    fine, coarse = (owner_ref, frank_ref), (ccell_ref, crank_ref)
    look_up(resp_ref, near, nf, nc, min(nc, 2), *coarse, left_ref, (cc_ref, ctr_ref))
    look_up(resp_ref, near, 0, nf, min(nf, 2), *fine, left_ref, (fc_ref, ftr_ref))
    await_tells(0, near)
    look_near(resp_ref, near, nf, nc, *coarse, (cc_ref, ctr_ref))
    look_near(resp_ref, near, 0, nf, *fine, (fc_ref, ftr_ref))
    blend(owner_ref.shape[0] // group_ref.shape[0], fc_ref, ftr_ref, cc_ref, ctr_ref, slab_ref)
    for k in range(1, n_level):
        join(k).start()
    slabs_ref[level] = slab_ref[level]
    each(1, n_dev, lambda k: ask(device(after(k)), me).wait_send())
    each(1, n_dev, lambda k: tell(device(after(k)), me).wait_send())
    for k in range(1, n_level):
        join(k).wait()
    rows = out_ref.shape[1]
    color, trans = slabs_ref[0, :rows, :], slabs_ref[0, rows:, :]
    for s in range(1, n_level):
        color = color + trans * slabs_ref[s, :rows, :]
        trans = trans * slabs_ref[s, rows:, :]
    out_ref[0] = color
    out_ref[1] = trans


def shards(
    coarse_density,
    coarse_emission,
    fine_density,
    fine_emission,
    coarse_brick,
    coarse_lane,
    coarse_entry,
    coarse_count,
    fine_owner,
    fine_brick,
    fine_lane,
    fine_entry,
    fine_count,
):
    n_morton = lax.axis_size("morton")
    n_level = lax.axis_size("level")
    n_dev = n_morton * n_level
    segments = fine_brick.shape[0]
    pixels = coarse_brick.shape[0]
    cap_f = -(-(2 * segments // n_dev) // LANES) * LANES
    cap_c = -(-pixels // (n_level * LANES)) * LANES
    nf, nc = cap_f // LANES, cap_c // LANES
    blocks = nf + nc
    f_rows, c_rows = segments // LANES, pixels // LANES
    level_rows = c_rows // n_level
    ints = [x.reshape(f_rows, LANES) for x in (fine_owner, fine_brick, fine_lane, fine_entry, fine_count)]
    ints += [x.reshape(c_rows, LANES) for x in (coarse_brick, coarse_lane, coarse_entry, coarse_count)]
    tables = [fine_density, fine_emission, coarse_density, coarse_emission]
    t_rows, g_rows = fine_density.shape[0], coarse_density.shape[0]
    wide = max(f_rows * n_dev, c_rows * n_morton)
    left_rows = 4 * n_dev * max(nf // min(nf, 2), nc // min(nc, 2))

    def like(x):
        return pltpu.VMEM(x.shape, x.dtype)

    sems = [pltpu.SemaphoreType.DMA((n_dev,))] * 4 + [pltpu.SemaphoreType.DMA((n_level,))] * 2
    image = pl.pallas_call(
        functools.partial(frame_kernel, n_morton, n_level, cap_f, cap_c),
        out_shape=jax.ShapeDtypeStruct((2, level_rows, LANES), F32),
        in_specs=[ANY] * 13,
        out_specs=VMEM,
        scratch_shapes=[like(x) for x in ints + tables]
        + [pltpu.VMEM((f_rows, LANES), I32)] * 5
        + [pltpu.VMEM((c_rows, LANES), I32)] * 5
        + [
            pltpu.VMEM((wide, LANES), BF16),
            pltpu.VMEM((wide, 2 * LANES), F32),
            pltpu.VMEM((4 * LANES, t_rows), BF16),
            pltpu.VMEM((-(-g_rows // LANES) * PER_ROW * 2 * BRICK, LANES), F32),
            pltpu.VMEM((left_rows, 2 * LANES), BF16),
        ]
        + [pltpu.VMEM((f_rows, LANES), F32)] * 2
        + [pltpu.VMEM((c_rows, LANES), F32)] * 2
        + [
            pltpu.VMEM((n_dev, blocks, LANES), I32),
            pltpu.VMEM((n_dev, blocks, LANES), I32),
            pltpu.VMEM((n_dev, 2 * blocks, LANES), F32),
            pltpu.VMEM((n_dev, 2 * blocks, LANES), F32),
            pltpu.VMEM((n_level, 2 * level_rows, LANES), F32),
            pltpu.VMEM((n_level, 2 * level_rows, LANES), F32),
        ]
        + sems
        + [pltpu.SemaphoreType.DMA((13,))]
        + [pltpu.VMEM((2 * LANES, cap_f), F32)] * 2,
        compiler_params=pltpu.CompilerParams(collective_id=0, has_side_effects=True),
    )(*ints, *tables)
    return image[0].reshape(-1), image[1].reshape(-1)


def solution(mesh):
    both = P(("morton", "level"))
    rows = P(("morton", "level"), None)
    coarse = P("morton", None)
    return jax.shard_map(
        shards,
        mesh=mesh,
        in_specs=(coarse, coarse, rows, rows, both, both, both, both, rows, both, both, both, both),
        out_specs=(both, both),
        check_vma=False,
    )
```

```python
import functools

import jax
import jax.numpy as jnp
from jax import lax
from jax.experimental import pallas as pl
from jax.experimental.pallas import tpu as pltpu
from jax.sharding import PartitionSpec as P

BRICK = 32
LANES = 128
SUBS = 8
PER_ROW = LANES // BRICK
COLUMNS = BRICK**2
F32 = jnp.float32
BF16 = jnp.bfloat16
I32 = jnp.int32
I16 = jnp.int16
VMEM = pl.BlockSpec(memory_space=pltpu.VMEM)
ANY = pl.BlockSpec(memory_space=pl.ANY)


def iota(shape, dim):
    return lax.broadcasted_iota(I32, shape, dim)


def equals(ids, width):
    return iota((width, ids.shape[1]), 0).astype(I16) == ids.astype(I16)


def onehot(ids, width):
    return jnp.where(equals(ids, width), jnp.ones((), BF16), jnp.zeros((), BF16))


def split(x, parts):
    out = []
    for _ in range(parts):
        piece = x.astype(BF16)
        out.append(piece)
        x = x - piece.astype(F32)
    return out


def dot_nt(a, b):
    return lax.dot_general(a, b, (((1,), (1,)), ((), ())), preferred_element_type=F32)


def dot_nn(a, b):
    return jnp.dot(a, b, preferred_element_type=F32)


def across(ref, at, rows):
    return jnp.concatenate([ref[at + r : at + r + 1, :] for r in range(rows)], axis=1)


def rank_rows(ids_ref, width, ones_ref, within_ref, out_ref):
    rows = ids_ref.shape[0]
    for r in range(rows):
        ones_ref[r * width : (r + 1) * width, :] = onehot(ids_ref[r : r + 1, :], width)
    lane, other = iota((LANES, 2 * LANES), 0), iota((LANES, 2 * LANES), 1)
    counter = jnp.where((lane < other) | (other >= LANES), 1.0, 0.0).astype(BF16)
    used = rows * width
    within_ref[:used, :] = dot_nn(ones_ref[:used, :], counter)
    ids_of = iota((width, LANES), 0)
    carry = jnp.zeros((width, LANES), F32)
    for r in range(rows):
        part = within_ref[r * width : (r + 1) * width, :]
        mine = jnp.where(ids_of == ids_ref[r : r + 1, :], part[:, :LANES] + carry, 0.0)
        out_ref[r : r + 1, :] = jnp.sum(mine, axis=0, keepdims=True).astype(I32)
        carry = carry + part[:, LANES:]


def to_float(value):
    return ((LANES + (value & (LANES - 1))) << (value >> 7)).astype(F32)


def from_float(x):
    y = x.astype(I32)
    shift = jnp.zeros_like(y)
    for bits in (8, 4, 2, 1):
        over = y >= (LANES << bits)
        y = jnp.where(over, y >> bits, y)
        shift = jnp.where(over, shift + bits, shift)
    return jnp.where(y == 0, 0, y - LANES + (shift << 7))


def place(cell_ref, lane_ref, code_ref, cells, chunk):
    rows = cell_ref.shape[0]
    placed = jnp.zeros((2 * cells, LANES), F32)
    for r in range(0, rows, chunk):
        here = equals(across(cell_ref, r, chunk), cells)
        code = across(code_ref, r, chunk)
        pieces = [to_float(code >> 11).astype(BF16), to_float(code & 2047).astype(BF16)]
        left = jnp.concatenate([jnp.where(here, p, jnp.zeros((), BF16)) for p in pieces], axis=0)
        right = onehot(across(lane_ref, r, chunk), LANES)
        placed = placed + dot_nt(left, right)
    return (from_float(placed[:cells]) << 11) + from_float(placed[cells:])


def cells_of(shape):
    rows = iota(shape, 0)
    return (rows & -BRICK) + 4 * (rows & 7) + ((rows >> 3) & 3)


def turned(turn, ref, parts):
    return [dot_nt(turn, piece) for piece in split(ref[...], parts)]


def turn_tables(ft_ref, fd_ref, fe_ref, ct_ref, cd_ref, ce_ref):
    turn = jnp.where(cells_of((LANES, LANES)) == iota((LANES, LANES), 1), 1.0, 0.0).astype(BF16)
    for at, ref in ((0, fd_ref), (LANES, fe_ref)):
        for i, piece in enumerate(turned(turn, ref, 2)):
            top = 2 * LANES * i + at
            ft_ref[top : top + LANES, :] = piece.astype(BF16)
    wide = ct_ref.shape[0] // PER_ROW
    rows = cd_ref.shape[0]
    for v, ref in enumerate((cd_ref, ce_ref)):
        whole = sum(turned(turn, ref, 3))
        for q in range(PER_ROW):
            for at in range(0, rows, LANES):
                size = min(LANES, rows - at)
                top = q * wide + (at // LANES) * 2 * BRICK + v * BRICK
                ct_ref[top : top + BRICK, :size] = whole[q * BRICK : (q + 1) * BRICK, at : at + size]


def fetch(codes, table_ref, got_ref):
    ones = onehot(codes >> 13, table_ref.shape[1])
    both = dot_nn(table_ref[...], ones)
    got_ref[...] = both[: 2 * LANES] + both[2 * LANES :]


def lanes_at(x, lanes):
    return jnp.take_along_axis(x, lanes, axis=1)


def front_to_back(dens, emis):
    trans = [jnp.exp(-d) for d in dens]
    color = [(1.0 - t) * e for t, e in zip(trans, emis)]
    c, t = color[3], trans[3]
    for k in (2, 1, 0):
        c = color[k] + trans[k] * c
        t = trans[k] * t
    for shift in (1, 2, 4):
        c = c + t * pltpu.roll(c, SUBS - shift, 0)
        t = t * pltpu.roll(t, SUBS - shift, 0)
    return c[0:1], t[0:1]


def march(codes, got_ref, at):
    codes = jnp.broadcast_to(codes, (SUBS, LANES))
    quarter = (codes >> 11) & (PER_ROW - 1)
    here = [quarter == q for q in range(PER_ROW - 1)]
    steps = BRICK // SUBS

    def column(top):
        out = []
        for k in range(steps):
            rows = [got_ref[top + q * BRICK + k * SUBS : top + q * BRICK + (k + 1) * SUBS, at : at + LANES] for q in range(PER_ROW)]
            x = rows[-1]
            for q in range(PER_ROW - 1):
                x = jnp.where(here[q], rows[q], x)
            out.append(x)
        return out

    return front_to_back(sampled(codes, column(0)), column(LANES))


def sampled(codes, dens):
    first = (codes >> 6) & (BRICK - 1)
    last = first + (codes & 63)
    steps = BRICK // SUBS
    cells = [steps * iota((SUBS, LANES), 0) + k for k in range(steps)]
    return [jnp.where((c >= first) & (c < last), x, 0.0) for c, x in zip(cells, dens)]


def march_lanes(codes, table_ref):
    codes = jnp.broadcast_to(codes, (SUBS, LANES))
    row = codes >> 13
    wide = table_ref.shape[0] // (PER_ROW * 2 * BRICK)
    group = ((codes >> 11) & (PER_ROW - 1)) * wide + row // LANES
    lane = row & (LANES - 1)
    got = [None] * (2 * BRICK // SUBS)
    for g in range(PER_ROW * wide):
        here = group == g
        for v in range(len(got)):
            top = g * 2 * BRICK + v * SUBS
            value = lanes_at(table_ref[top : top + SUBS, :], lane)
            got[v] = value if g == 0 else jnp.where(here, value, got[v])
    steps = BRICK // SUBS
    return front_to_back(sampled(codes, got[:steps]), got[steps:])


def look_up(resp_ref, low, at, blocks, width, owner_ref, rank_ref, left_ref, out_refs):
    half = resp_ref.shape[1] // 2
    owners = resp_ref.shape[0] - low
    high = blocks // width
    cells = high * owners
    for v in range(2):
        for h in range(high):
            for w in range(width):
                full = resp_ref[low:, v * half + at + h * width + w, :]
                for i, piece in enumerate(split(full, 2)):
                    top = (2 * v + i) * cells + h * owners
                    left_ref[top : top + owners, w * LANES : (w + 1) * LANES] = piece
    chunk = SUBS
    left = left_ref[: 4 * cells, : width * LANES]
    for r in range(0, owner_ref.shape[0], chunk):
        owner, rank = across(owner_ref, r, chunk), across(rank_ref, r, chunk)
        got = dot_nn(left, onehot(rank & (width * LANES - 1), width * LANES))
        cell = jnp.where(owner >= low, owner - low + rank // (width * LANES) * owners, -1)
        here = iota((cells, chunk * LANES), 0) == cell
        for v in range(2):
            total = got[2 * v * cells : (2 * v + 1) * cells] + got[(2 * v + 1) * cells : (2 * v + 2) * cells]
            value = jnp.sum(jnp.where(here, total, 0.0), axis=0, keepdims=True)
            for j in range(chunk):
                out_refs[v][r + j : r + j + 1, :] += value[:, j * LANES : (j + 1) * LANES]


def look_near(resp_ref, low, owners, at, blocks, owner_ref, rank_ref, out_refs):
    half = resp_ref.shape[1] // 2
    for r in range(0, owner_ref.shape[0], SUBS):
        rank = rank_ref[r : r + SUBS, :]
        cell = (owner_ref[r : r + SUBS, :] - low) * blocks + rank // LANES
        lane = rank & (LANES - 1)
        values = [ref[r : r + SUBS, :] for ref in out_refs]
        for d in range(owners):
            for b in range(blocks):
                here = cell == d * blocks + b
                for v in range(2):
                    top = v * half + at + b
                    row = resp_ref[low + d, top : top + 1, :]
                    value = lanes_at(jnp.broadcast_to(row, (SUBS, LANES)), lane)
                    values[v] = jnp.where(here, value, values[v])
        for ref, value in zip(out_refs, values):
            ref[r : r + SUBS, :] = value


def blend(per_pixel, fine_c, fine_t, coarse_c, coarse_t, slab_ref):
    rows = fine_c.shape[0]
    level_rows = slab_ref.shape[1] // 2
    pixel_lanes = LANES // per_pixel
    lane = iota((SUBS, LANES), 1)
    source = (lane & (pixel_lanes - 1)) * per_pixel
    group = lane // pixel_lanes
    for r in range(0, rows, SUBS):
        c, t = fine_c[r : r + SUBS, :], fine_t[r : r + SUBS, :]
        shift = 1
        while shift < per_pixel:
            c = c + t * pltpu.roll(c, LANES - shift, 1)
            t = t * pltpu.roll(t, LANES - shift, 1)
            shift *= 2
        c, t = lanes_at(c, source), lanes_at(t, source)
        c, t = jnp.take_along_axis(c, group, axis=0)[0:1], jnp.take_along_axis(t, group, axis=0)[0:1]
        row = r // SUBS
        c0, t0 = coarse_c[row : row + 1, :], coarse_t[row : row + 1, :]
        to, at = row // level_rows, row % level_rows
        slab_ref[to, at : at + 1, :] = c0 + t0 * c
        slab_ref[to, level_rows + at : level_rows + at + 1, :] = t0 * t


def frame_kernel(n_morton, n_level, cap_f, cap_c, *refs):
    ints, tables, out_ref, refs = refs[:9], refs[9:13], refs[13], refs[14:]
    int_refs, table_refs, refs = refs[:9], refs[9:13], refs[13:]
    (
        owner_ref,
        fcode_ref,
        frank_ref,
        fcell_ref,
        flane_ref,
        group_ref,
        ccode_ref,
        crank_ref,
        ccell_ref,
        clane_ref,
        ones_ref,
        within_ref,
        ft_ref,
        ct_ref,
        left_ref,
        fc_ref,
        ftr_ref,
        cc_ref,
        ctr_ref,
        msg_ref,
        code_ref,
        served_ref,
        resp_ref,
        slab_ref,
        slabs_ref,
        ask_send,
        ask_recv,
        tell_send,
        tell_recv,
        join_send,
        join_recv,
        in_sems,
        *refs,
    ) = refs
    bufs = refs
    n_dev = n_morton * n_level
    nf, nc = cap_f // LANES, cap_c // LANES
    blocks = nf + nc
    copies = [
        pltpu.make_async_copy(src, dst, in_sems.at[i])
        for i, (src, dst) in enumerate(zip(ints + tables, int_refs + table_refs))
    ]
    for copy in copies[:9]:
        copy.start()
    morton, level = lax.axis_index("morton"), lax.axis_index("level")
    me = morton * n_level + level
    mesh_ids = pl.DeviceIdType.MESH

    def device(d):
        return d // n_level, lax.rem(d, n_level)

    def wrap(x, n):
        return jnp.where(x >= n, x - n, x)

    def others(act):
        levels = [wrap(level + k, n_level) for k in range(n_level)]
        for there in levels[1:]:
            act(morton, there)

        def group(k, _):
            for there in levels:
                act(wrap(morton + k, n_morton), there)
            return 0

        lax.fori_loop(1, n_morton, group, 0)

    def ask(there, source):
        return pltpu.make_async_remote_copy(
            src_ref=msg_ref.at[there[0] * n_level + there[1]],
            dst_ref=code_ref.at[me],
            send_sem=ask_send.at[there[0] * n_level + there[1]],
            recv_sem=ask_recv.at[source],
            device_id=there,
            device_id_type=mesh_ids,
        )

    def tell(there, source):
        return pltpu.make_async_remote_copy(
            src_ref=served_ref.at[there[0] * n_level + there[1]],
            dst_ref=resp_ref.at[source],
            send_sem=tell_send.at[there[0] * n_level + there[1]],
            recv_sem=tell_recv.at[source],
            device_id=there,
            device_id_type=mesh_ids,
        )

    ordered = n_morton % 2 == 0 and n_morton >= 6 and n_level % 2 == 0
    near = 2 * n_level
    partner = level + 1 - 2 * lax.rem(level, 2)
    row, column_in = morton // 2, lax.rem(morton, 2)
    start = row * near if ordered else 0

    def seen_by(d, m):
        return wrap(d + n_dev - m // 2 * near, n_dev) if ordered else d

    def source(t):
        if not ordered:
            return lax.rem(me + n_dev - t, n_dev)
        n_rows = n_morton // 2
        step = jnp.maximum(t - n_level, 0)
        g, turn = step // n_level, lax.rem(step, n_level)
        first = row == 0
        u = jnp.maximum(jnp.where(first, g - 1, g - 2), 0)
        down = jnp.maximum(n_rows - 2 - u // 2, 0)
        far = 2 * (1 + jnp.where(row == 1, down, lax.rem(row + u // 2, n_rows - 1))) + lax.rem(u + 1 + column_in, 2)
        head = jnp.where(first, g < 1, g < 2)
        group = jnp.where(head, jnp.where(first, 1 - column_in, g), far)
        group = jnp.where((row > 0) & (g == n_morton - 2), 2 * row + 1 - column_in, group)
        i = jnp.maximum(t - 2, 0)
        beside = lax.rem(jnp.where(lax.rem(i, 2) == 0, level, partner) + 2 * (i // 2 + 1), n_level)
        same = jnp.where(lax.rem(turn, 2) == 0, level, partner)
        away = group * n_level + lax.rem(same + n_level - 2 * (turn // 2 + 1), n_level)
        far_or_beside = jnp.where(t < n_level, morton * n_level + beside, away)
        return jnp.where(t == 0, me, jnp.where(t == 1, morton * n_level + partner, far_or_beside))

    def join(k):
        to = lax.rem(level + k, n_level)
        return pltpu.make_async_remote_copy(
            src_ref=slab_ref.at[to],
            dst_ref=slabs_ref.at[level],
            send_sem=join_send.at[k],
            recv_sem=join_recv.at[k],
            device_id=(morton, to),
            device_id_type=mesh_ids,
        )

    def after(k):
        return wrap(me + k, n_dev)

    barrier = pltpu.get_barrier_semaphore()

    def each(low, high, act):
        def body(k, _):
            act(k)
            return 0

        lax.fori_loop(low, high, body, 0)

    def greet(m, _):
        for k in range(n_level):
            there = wrap(level + k, n_level)

            def one():
                pl.semaphore_signal(barrier, inc=1, device_id=(m, there), device_id_type=mesh_ids)

            one() if k else pl.when(m != morton)(one)
        return 0

    lax.fori_loop(0, n_morton, greet, 0)
    for copy in copies[9:]:
        copy.start()
    for copy in copies[:9]:
        copy.wait()
    f_owner, f_brick, f_lane, f_entry, f_count, c_brick, c_lane, c_entry, c_count = int_refs

    owner_ref[...] = f_owner[...]
    fcode_ref[...] = (((f_brick[...] * COLUMNS + f_lane[...]) * BRICK + f_entry[...]) << 6) + f_count[...]
    rank_rows(owner_ref, n_dev, ones_ref, within_ref, frank_ref)
    rank = frank_ref[...]
    fcell_ref[...] = f_owner[...] * nf + rank // LANES
    flane_ref[...] = rank & (LANES - 1)
    fine_msg = place(fcell_ref, flane_ref, fcode_ref, n_dev * nf, SUBS)

    c_cols = table_refs[2].shape[0] * PER_ROW
    column = c_brick[...] * COLUMNS + c_lane[...]
    group_ref[...] = column // c_cols
    ccode_ref[...] = (((column & (c_cols - 1)) * BRICK + c_entry[...]) << 6) + c_count[...]
    rank_rows(group_ref, n_morton, ones_ref, within_ref, crank_ref)
    rank = crank_ref[...]
    slot = rank // n_level
    dest = group_ref[...] * n_level + (rank & (n_level - 1))
    ccell_ref[...] = dest * nc + slot // LANES
    clane_ref[...] = slot & (LANES - 1)
    coarse_msg = place(ccell_ref, clane_ref, ccode_ref, n_dev * nc, SUBS)
    for i in range(n_dev):
        msg_ref[i, :nf, :] = fine_msg[i * nf : (i + 1) * nf]
        msg_ref[i, nf:, :] = coarse_msg[i * nc : (i + 1) * nc]

    pl.semaphore_wait(barrier, n_dev - 1)
    others(lambda m, l: ask((m, l), me).start())
    pltpu.make_async_copy(msg_ref.at[me], code_ref.at[me], ask_recv.at[me]).start()
    for copy in copies[9:]:
        copy.wait()
    fd_ref, fe_ref, cd_ref, ce_ref = table_refs
    turn_tables(ft_ref, fd_ref, fe_ref, ct_ref, cd_ref, ce_ref)

    def codes_of(i, at, rows):
        return jnp.concatenate([code_ref[i, at + r : at + r + 1, :] for r in range(rows)], axis=1)

    def put(i, b, c, t):
        served_ref[i, b : b + 1, :] = c
        served_ref[i, blocks + b : blocks + b + 1, :] = t

    def fetch_source(i, buf):
        fetch(codes_of(i, 0, nf), ft_ref, buf)
        for b in range(nf, blocks):
            put(i, b, *march_lanes(code_ref[i, b : b + 1, :], ct_ref))

    def march_source(i, buf):
        for b in range(nf):
            put(i, b, *march(code_ref[i, b : b + 1, :], buf, b * LANES))

    bufs[-1][...] = jnp.zeros(bufs[-1].shape, F32)

    def await_ask(d):
        ask((morton, level), d).wait_recv()

    def start_tell(d):
        there = device(d)
        tell(there, seen_by(me, there[0])).start()

    def march_some(now, last, last_buf):
        for d in now:
            await_ask(d)
        spare = [b for b in bufs if b is not last_buf]
        for i, d in enumerate(now):
            buf = bufs[-1] if i == len(now) - 1 else spare[i]
            fetch_source(d, buf)
            march_source(now[i - 1] if i else last, spare[i - 1] if i else last_buf)

    by = len(bufs)
    first = tuple(source(i) for i in range(2))
    march_some(first, me, bufs[-1])

    def some_sources(j, state):
        marched, last, now = state

        @pl.when(j > 0)
        def _():
            for d in marched:
                start_tell(d)

        march_some(now, last, bufs[-1])
        ahead = jnp.minimum(by * (j + 1) + 2, n_dev - by)
        return (last, *now[:-1]), now[-1], tuple(source(ahead + i) for i in range(by))

    bodies = (n_dev - 2) // by
    state = ((me,) * by, first[-1], tuple(source(2 + i) for i in range(by)))
    marched, last, _ = lax.fori_loop(0, bodies, some_sources, state)
    for d in marched:
        start_tell(d)
    rest = tuple(source(t) for t in range(by * bodies + 2, n_dev))
    if rest:
        march_some(rest, last, bufs[-1])
        for d in (last, *rest[:-1]):
            start_tell(d)
        last = rest[-1]
    march_source(last, bufs[-1])
    start_tell(last)
    mine = seen_by(me, morton)
    resp_ref[mine] = served_ref[me]
    seen = owner_ref[...] - start
    owner_ref[...] = jnp.where(seen < 0, seen + n_dev, seen)
    rank = crank_ref[...]
    seen = group_ref[...] * n_level + (rank & (n_level - 1)) - start
    ccell_ref[...] = jnp.where(seen < 0, seen + n_dev, seen)
    crank_ref[...] = rank // n_level
    for ref in (fc_ref, ftr_ref, cc_ref, ctr_ref):
        ref[...] = jnp.zeros(ref.shape, F32)

    def await_tells(low, high):
        def one(v, _):
            @pl.when(v != mine)
            def _():
                tell((morton, level), v).wait_recv()

            return 0

        lax.fori_loop(low, high, one, 0)

    fine, coarse = (owner_ref, frank_ref), (ccell_ref, crank_ref)

    def take_near(low, owners):
        look_near(resp_ref, low, owners, nf, nc, *coarse, (cc_ref, ctr_ref))
        look_near(resp_ref, low, owners, 0, nf, *fine, (fc_ref, ftr_ref))

    past = 2 * near if ordered else 0
    await_tells(past, n_dev)
    if ordered:
        own = column_in * n_level
        await_tells(own, own + n_level)
        take_near(own, n_level)
    look_up(resp_ref, past, nf, nc, min(nc, 2), *coarse, left_ref, (cc_ref, ctr_ref))
    look_up(resp_ref, past, 0, nf, min(nf, 2), *fine, left_ref, (fc_ref, ftr_ref))
    if ordered:
        await_tells(near, past)
        take_near(near, near)
        beside_own = (1 - column_in) * n_level
        await_tells(beside_own, beside_own + n_level)
        take_near(beside_own, n_level)
    blend(owner_ref.shape[0] // group_ref.shape[0], fc_ref, ftr_ref, cc_ref, ctr_ref, slab_ref)
    for k in range(1, n_level):
        join(k).start()
    slabs_ref[level] = slab_ref[level]
    each(1, n_dev, lambda k: ask(device(after(k)), me).wait_send())
    each(1, n_dev, lambda k: tell(device(after(k)), me).wait_send())
    for k in range(1, n_level):
        join(k).wait()
    rows = out_ref.shape[1]
    color, trans = slabs_ref[0, :rows, :], slabs_ref[0, rows:, :]
    for s in range(1, n_level):
        color = color + trans * slabs_ref[s, :rows, :]
        trans = trans * slabs_ref[s, rows:, :]
    out_ref[0] = color
    out_ref[1] = trans


def shards(
    coarse_density,
    coarse_emission,
    fine_density,
    fine_emission,
    coarse_brick,
    coarse_lane,
    coarse_entry,
    coarse_count,
    fine_owner,
    fine_brick,
    fine_lane,
    fine_entry,
    fine_count,
):
    n_morton = lax.axis_size("morton")
    n_level = lax.axis_size("level")
    n_dev = n_morton * n_level
    segments = fine_brick.shape[0]
    pixels = coarse_brick.shape[0]
    cap_f = -(-(2 * segments // n_dev) // LANES) * LANES
    cap_c = -(-pixels // (n_level * LANES)) * LANES
    nf, nc = cap_f // LANES, cap_c // LANES
    blocks = nf + nc
    f_rows, c_rows = segments // LANES, pixels // LANES
    level_rows = c_rows // n_level
    ints = [x.reshape(f_rows, LANES) for x in (fine_owner, fine_brick, fine_lane, fine_entry, fine_count)]
    ints += [x.reshape(c_rows, LANES) for x in (coarse_brick, coarse_lane, coarse_entry, coarse_count)]
    tables = [fine_density, fine_emission, coarse_density, coarse_emission]
    t_rows, g_rows = fine_density.shape[0], coarse_density.shape[0]
    wide = max(f_rows * n_dev, c_rows * n_morton)

    def like(x):
        return pltpu.VMEM(x.shape, x.dtype)

    sems = [pltpu.SemaphoreType.DMA((n_dev,))] * 4 + [pltpu.SemaphoreType.DMA((n_level,))] * 2
    image = pl.pallas_call(
        functools.partial(frame_kernel, n_morton, n_level, cap_f, cap_c),
        out_shape=jax.ShapeDtypeStruct((2, level_rows, LANES), F32),
        in_specs=[ANY] * 13,
        out_specs=VMEM,
        scratch_shapes=[like(x) for x in ints + tables]
        + [pltpu.VMEM((f_rows, LANES), I32)] * 5
        + [pltpu.VMEM((c_rows, LANES), I32)] * 5
        + [
            pltpu.VMEM((wide, LANES), BF16),
            pltpu.VMEM((wide, 2 * LANES), F32),
            pltpu.VMEM((4 * LANES, t_rows), BF16),
            pltpu.VMEM((-(-g_rows // LANES) * PER_ROW * 2 * BRICK, LANES), F32),
            pltpu.VMEM((4 * n_dev * max(nf // min(nf, 2), nc // min(nc, 2)), 2 * LANES), BF16),
        ]
        + [pltpu.VMEM((f_rows, LANES), F32)] * 2
        + [pltpu.VMEM((c_rows, LANES), F32)] * 2
        + [
            pltpu.VMEM((n_dev, blocks, LANES), I32),
            pltpu.VMEM((n_dev, blocks, LANES), I32),
            pltpu.VMEM((n_dev, 2 * blocks, LANES), F32),
            pltpu.VMEM((n_dev, 2 * blocks, LANES), F32),
            pltpu.VMEM((n_level, 2 * level_rows, LANES), F32),
            pltpu.VMEM((n_level, 2 * level_rows, LANES), F32),
        ]
        + sems
        + [pltpu.SemaphoreType.DMA((13,))]
        + [pltpu.VMEM((2 * LANES, cap_f), F32)] * min(4, n_dev - 2),
        compiler_params=pltpu.CompilerParams(collective_id=0, has_side_effects=True),
    )(*ints, *tables)
    return image[0].reshape(-1), image[1].reshape(-1)


def solution(mesh):
    both = P(("morton", "level"))
    rows = P(("morton", "level"), None)
    coarse = P("morton", None)
    return jax.shard_map(
        shards,
        mesh=mesh,
        in_specs=(coarse, coarse, rows, rows, both, both, both, both, rows, both, both, both, both),
        out_specs=(both, both),
        check_vma=False,
    )
```
